8 devices in a mesh: dp: 1 (over z), sp: 8 (over y, x, core).
Axes of the slice: x: 2, y: 2, z: 1, core: 2. Of those that a mesh axis runs over, the one named last changes fastest.
Arguments:
- x: bfloat16 [8, 2048, 1024], P('dp', 'sp')
- ln1_gain: bfloat16 [1024], replicated
- ln1_bias: bfloat16 [1024], replicated
- w_query: bfloat16 [1024, 1024], replicated
- b_query: bfloat16 [1024], replicated
- w_key: bfloat16 [1024, 1024], replicated
- w_value: bfloat16 [1024, 1024], replicated
- b_value: bfloat16 [1024], replicated
- w_out: bfloat16 [1024, 1024], replicated
- b_out: bfloat16 [1024], replicated
- ln2_gain: bfloat16 [1024], replicated
- ln2_bias: bfloat16 [1024], replicated
- w_up: bfloat16 [1024, 4096], replicated
- b_up: bfloat16 [4096], replicated
- w_down: bfloat16 [4096, 1024], replicated
- b_down: bfloat16 [1024], replicated
- lnp_gain: bfloat16 [1024], replicated
- lnp_bias: bfloat16 [1024], replicated
- cross_wk: bfloat16 [2, 1024, 1024], P(None, None, 'sp')
- cross_wv: bfloat16 [2, 1024, 1024], P(None, None, 'sp')
- cross_bv: bfloat16 [2, 1024], P(None, 'sp')
Outputs:
- output 1: bfloat16 [2, 8, 2048, 16, 64], P(None, 'dp', None, 'sp')
- output 2: bfloat16 [2, 8, 2048, 16, 64], P(None, 'dp', None, 'sp')
All inputs are finite; a program needn't handle non-finite values.
Results may differ from the reference program's by a relative error of at most 0.00748584.
Values are sent between devices in bfloat16 or wider.
A program may use at most 1 GiB of HBM per device.

```python
import math
import jax
import jax.numpy as jnp
from jax import lax

BATCH_SIZE = 8
FRAMES = 2048
D_MODEL = 1024
NUM_HEADS = 16
FF_DIM = 4096
DEC_LAYERS = 2
HEAD_DIM = D_MODEL // NUM_HEADS


def normal_draw(rng_key, dims, std_dev):
    return (jax.random.normal(rng_key, dims, jnp.float32) * std_dev).astype(jnp.bfloat16)


def gain_draw(rng_key, width):
    return (1.0 + 0.2 * jax.random.normal(rng_key, (width,), jnp.float32)).astype(jnp.bfloat16)


def setup_inputs(seed: int = 0, part: int = 0) -> dict:
    base_key = jax.random.key(seed)
    part_key = jax.random.fold_in(base_key, part)
    key_list = jax.random.split(base_key, 20)
    score_std = math.sqrt(math.log(FRAMES / 4.0))
    qk_std = math.sqrt(score_std / D_MODEL)
    out_std = D_MODEL ** -0.5
    return {
        'x': normal_draw(part_key, (BATCH_SIZE, FRAMES, D_MODEL), 1.0),
        'ln1_gain': gain_draw(key_list[0], D_MODEL),
        'ln1_bias': normal_draw(key_list[1], (D_MODEL,), 0.2),
        'w_query': normal_draw(key_list[2], (D_MODEL, D_MODEL), qk_std),
        'b_query': normal_draw(key_list[3], (D_MODEL,), 0.5 * math.sqrt(score_std)),
        'w_key': normal_draw(key_list[4], (D_MODEL, D_MODEL), qk_std),
        'w_value': normal_draw(key_list[5], (D_MODEL, D_MODEL), out_std),
        'b_value': normal_draw(key_list[6], (D_MODEL,), 0.5),
        'w_out': normal_draw(key_list[7], (D_MODEL, D_MODEL), out_std),
        'b_out': normal_draw(key_list[8], (D_MODEL,), 0.3),
        'ln2_gain': gain_draw(key_list[9], D_MODEL),
        'ln2_bias': normal_draw(key_list[10], (D_MODEL,), 0.2),
        'w_up': normal_draw(key_list[11], (D_MODEL, FF_DIM), out_std),
        'b_up': normal_draw(key_list[12], (FF_DIM,), 0.5),
        'w_down': normal_draw(key_list[13], (FF_DIM, D_MODEL), FF_DIM ** -0.5),
        'b_down': normal_draw(key_list[14], (D_MODEL,), 0.3),
        'lnp_gain': gain_draw(key_list[15], D_MODEL),
        'lnp_bias': normal_draw(key_list[16], (D_MODEL,), 0.2),
        'cross_wk': normal_draw(key_list[17], (DEC_LAYERS, D_MODEL, D_MODEL), out_std),
        'cross_wv': normal_draw(key_list[18], (DEC_LAYERS, D_MODEL, D_MODEL), out_std),
        'cross_bv': normal_draw(key_list[19], (DEC_LAYERS, D_MODEL), 0.5),
    }


def layer_norm(hidden_in, ln_gain, ln_bias):
    mean_val = jnp.mean(hidden_in, axis=-1, keepdims=True)
    centered = hidden_in - mean_val
    variance = jnp.mean(centered * centered, axis=-1, keepdims=True)
    return centered * lax.rsqrt(variance + 1e-5) * ln_gain.astype(jnp.float32) + ln_bias.astype(jnp.float32)


def reference(x, ln1_gain, ln1_bias, w_query, b_query, w_key, w_value, b_value, w_out, b_out, ln2_gain, ln2_bias, w_up, b_up, w_down, b_down, lnp_gain, lnp_bias, cross_wk, cross_wv, cross_bv):
    qk_scale = HEAD_DIM ** -0.25
    row_count = BATCH_SIZE * FRAMES
    residual = x.astype(jnp.float32).reshape(row_count, D_MODEL)
    normed = layer_norm(residual, ln1_gain, ln1_bias).astype(jnp.bfloat16)
    queries = ((jnp.dot(normed, w_query, preferred_element_type=jnp.float32) + b_query.astype(jnp.float32)) * qk_scale).astype(jnp.bfloat16)
    key_rows = (jnp.dot(normed, w_key, preferred_element_type=jnp.float32) * qk_scale).astype(jnp.bfloat16)
    value_rows = (jnp.dot(normed, w_value, preferred_element_type=jnp.float32) + b_value.astype(jnp.float32)).astype(jnp.bfloat16)

    def split_heads(rows_in):
        return rows_in.reshape(BATCH_SIZE, FRAMES, NUM_HEADS, HEAD_DIM).transpose(0, 2, 1, 3).reshape(BATCH_SIZE * NUM_HEADS, FRAMES, HEAD_DIM)

    def head_attention(operands):
        q_head, k_head, v_head = operands
        scores = jnp.dot(q_head, k_head.T, preferred_element_type=jnp.float32)
        attn_probs = jax.nn.softmax(scores, axis=-1).astype(jnp.bfloat16)
        return jnp.dot(attn_probs, v_head, preferred_element_type=jnp.float32).astype(jnp.bfloat16)

    attended = lax.map(head_attention, (split_heads(queries), split_heads(key_rows), split_heads(value_rows)))
    attended = attended.reshape(BATCH_SIZE, NUM_HEADS, FRAMES, HEAD_DIM).transpose(0, 2, 1, 3).reshape(row_count, D_MODEL)
    residual = residual + jnp.dot(attended, w_out, preferred_element_type=jnp.float32) + b_out.astype(jnp.float32)
    normed = layer_norm(residual, ln2_gain, ln2_bias).astype(jnp.bfloat16)
    hidden = jax.nn.gelu(jnp.dot(normed, w_up, preferred_element_type=jnp.float32) + b_up.astype(jnp.float32), approximate=False).astype(jnp.bfloat16)
    residual = residual + jnp.dot(hidden, w_down, preferred_element_type=jnp.float32) + b_down.astype(jnp.float32)
    y_rows = layer_norm(residual, lnp_gain, lnp_bias).astype(jnp.bfloat16)

    def layer_cache(layer_weights):
        wk_layer, wv_layer, bv_layer = layer_weights
        k_layer = jnp.dot(y_rows, wk_layer, preferred_element_type=jnp.float32).astype(jnp.bfloat16)
        v_layer = (jnp.dot(y_rows, wv_layer, preferred_element_type=jnp.float32) + bv_layer.astype(jnp.float32)).astype(jnp.bfloat16)
        return k_layer, v_layer

    k_all, v_all = lax.map(layer_cache, (cross_wk, cross_wv, cross_bv))
    cache_shape = (DEC_LAYERS, BATCH_SIZE, FRAMES, NUM_HEADS, HEAD_DIM)
    return k_all.reshape(cache_shape), v_all.reshape(cache_shape)
```

```python
import functools
import math

import jax
import jax.numpy as jnp
from jax import lax
from jax.experimental import pallas as pl
from jax.experimental.pallas import tpu as pltpu
from jax.sharding import PartitionSpec as P

HEAD_DIM = 64
LN_EPS = 1e-5
LOG2E = math.log2(math.e)
V_ROWS = 80
F32 = jnp.float32
BF16 = jnp.bfloat16


def layer_norm(h, gain, bias):
    mean = jnp.mean(h, axis=-1, keepdims=True)
    centered = h - mean
    var = jnp.mean(centered * centered, axis=-1, keepdims=True)
    return centered * lax.rsqrt(var + LN_EPS) * gain + bias


def wide(row):
    return row.astype(F32).reshape(1, -1)


def dot(a, b, ca=1, cb=0):
    return lax.dot_general(a, b, (((ca,), (cb,)), ((), ())), preferred_element_type=F32)


def encoder_kernel(
    x_hbm, wq_hbm, wk_hbm, wv_hbm, wo_hbm, w1_hbm, w2_hbm,
    g1_ref, c1_ref, bq_ref, bv_ref, bo_ref, g2_ref, c2_ref, b1_ref, b2_ref, gp_ref, cp_ref,
    y_hbm,
    xc, wq, wk, wv, wo, w1, w2, q_s, k_s, v_s, sa, sb, o_s, y_s,
    x_send, x_recv, y_send, f_send, y_recv, load_sem, y_loc,
    *, n_dev, rows,
):
    d_model = wq.shape[0]
    d_ff = w1.shape[1]
    pairs = d_model // 128
    frames = n_dev * rows
    scale = HEAD_DIM**-0.25
    me = lax.axis_index("sp")
    core = me % 2
    px = (me // 2) % 2
    py = me // 4

    def flip(t):
        c = core + (t % 2) * (1 - 2 * core)
        x = px + ((t // 2) % 2) * (1 - 2 * px)
        y = py + (t // 4) * (1 - 2 * py)
        return y * 4 + x * 2 + c

    near, across_x, across_y, diag = flip(1), flip(2), flip(4), flip(6)

    barrier = pltpu.get_barrier_semaphore()
    for t in range(1, n_dev):
        pl.semaphore_signal(barrier, inc=1, device_id={"sp": flip(t)}, device_id_type=pl.DeviceIdType.MESH)
    pl.semaphore_wait(barrier, n_dev - 1)

    def x_copy(dst_dev, t):
        return pltpu.make_async_remote_copy(
            src_ref=x_hbm.at[dst_dev], dst_ref=xc.at[me], send_sem=x_send.at[t], recv_sem=x_recv.at[me],
            device_id={"sp": dst_dev}, device_id_type=pl.DeviceIdType.MESH,
        )

    def x_arrival(src):
        return pltpu.make_async_remote_copy(
            src_ref=x_hbm.at[src], dst_ref=xc.at[src], send_sem=x_send.at[0], recv_sem=x_recv.at[src],
            device_id={"sp": near}, device_id_type=pl.DeviceIdType.MESH,
        )

    own_x = pltpu.make_async_copy(x_hbm.at[me], xc.at[me], load_sem.at[0])
    own_x.start()
    for t in (2, 4, 3, 5, 6, 7, 1):
        x_copy(flip(t), t).start()
    loads = [
        pltpu.make_async_copy(a, b, load_sem.at[i + 1])
        for i, (a, b) in enumerate(
            ((wq_hbm, wq), (wk_hbm, wk), (wv_hbm, wv), (wo_hbm, wo), (w1_hbm, w1), (w2_hbm, w2))
        )
    ]
    for c in loads:
        c.start()

    ones = (lax.broadcasted_iota(jnp.int32, (V_ROWS - HEAD_DIM, frames), 0) == 0).astype(BF16)
    for h in range(2 * pairs):
        v_s[h, HEAD_DIM:, :] = ones

    own_x.wait()
    for c in loads[:3]:
        c.wait()

    def project(t, carry):
        src = flip(t)

        @pl.when(t > 0)
        def _():
            x_arrival(src).wait_recv()

        a = layer_norm(xc[src].astype(F32), wide(g1_ref[...]), wide(c1_ref[...])).astype(BF16)
        at = pl.multiple_of(src * rows, rows)
        q = ((dot(a, wq[...]) + wide(bq_ref[...])) * scale).astype(BF16)
        k = (dot(a, wk[...]) * scale).astype(BF16)
        for p in range(pairs):
            q_s[p, pl.ds(at, rows), :] = q[:, p * 128 : (p + 1) * 128]
            k_s[p, pl.ds(at, rows), :] = k[:, p * 128 : (p + 1) * 128]
        v = (dot(a, wv[...]) + wide(bv_ref[...])).astype(BF16).T
        for h in range(2 * pairs):
            v_s[h, :HEAD_DIM, pl.ds(at, rows)] = v[h * HEAD_DIM : (h + 1) * HEAD_DIM]
        return carry

    lax.fori_loop(0, n_dev, project, 0)
    for c in loads[3:]:
        c.wait()

    lane = lax.broadcasted_iota(jnp.int32, (rows, 128), 1)
    kc = 512

    def y_copy(src_ref, src, j, dst_dev, sem):
        return pltpu.make_async_remote_copy(
            src_ref=src_ref, dst_ref=y_hbm.at[src, pl.ds(pl.multiple_of(j * rows, rows), rows)],
            send_sem=sem, recv_sem=y_recv.at[src, j],
            device_id={"sp": dst_dev}, device_id_type=pl.DeviceIdType.MESH,
        )

    def y_block(src, j):
        return y_hbm.at[src, pl.ds(pl.multiple_of(j * rows, rows), rows)]

    def forward(src, j, dst_dev, kind):
        return y_copy(y_block(src, j), src, j, dst_dev, f_send.at[kind, j])

    def arrived(src, j):
        y_copy(y_block(src, j), src, j, near, f_send.at[0, j]).wait_recv()

    def own(j, kind, dst_dev):
        return y_copy(y_s.at[j % 2], me, j, dst_dev, y_send.at[kind, j % 2])

    def store_own(j):
        return pltpu.make_async_copy(y_s.at[j % 2], y_block(me, j), y_loc.at[j % 2])

    def relay_first(j):
        arrived(across_x, j)
        arrived(across_y, j)
        forward(across_x, j, near, 0).start()
        forward(across_y, j, near, 1).start()
        via, to = (1 - core) * across_x + core * across_y, (1 - core) * across_y + core * across_x
        forward(via, j, to, 2).start()

    def relay_second(j):
        arrived(diag, j)
        forward(diag, j, near, 3).start()

    def scores(q_pair, pair, parity, s_ref, c, mx):
        q = jnp.where((lane < HEAD_DIM) if parity == 0 else (lane >= HEAD_DIM), q_pair, jnp.zeros_like(q_pair))
        s = dot(k_s[pair, c * kc : (c + 1) * kc, :], q, 1, 1)
        s_ref[c * kc : (c + 1) * kc, :] = s
        return jnp.maximum(mx, jnp.max(s.reshape(kc // 8, 8, rows), axis=0))

    mx0 = jnp.full((8, rows), -jnp.inf, F32)

    def step(j, carry):
        at = pl.multiple_of(j * rows, rows)

        def head(pair, parity, cur, nxt, next_pair, mx):
            m = jnp.max(mx, axis=0, keepdims=True) * LOG2E
            q_pair = q_s[next_pair, pl.ds(at, rows), :]
            new_mx = mx0
            o = jnp.zeros((V_ROWS, rows), F32)
            for c in range(frames // kc):
                new_mx = scores(q_pair, next_pair, 1 - parity, nxt, c, new_mx)
                p = jnp.exp2(cur[c * kc : (c + 1) * kc, :] * LOG2E - m).astype(BF16)
                o = o + dot(v_s[2 * pair + parity, :, c * kc : (c + 1) * kc], p)
            o = (o[:HEAD_DIM] * (1.0 / o[HEAD_DIM : HEAD_DIM + 1])).astype(BF16)
            o_s[pl.ds(pl.multiple_of(pair * 128 + parity * HEAD_DIM, HEAD_DIM), HEAD_DIM), :] = o
            return new_mx

        mx = mx0
        for c in range(frames // kc):
            mx = scores(q_s[0, pl.ds(at, rows), :], 0, 0, sa, c, mx)

        def two_heads(pair, mx):
            mx = head(pair, 0, sa, sb, pair, mx)
            return head(pair, 1, sb, sa, jnp.minimum(pair + 1, pairs - 1), mx)

        lax.fori_loop(0, pairs, two_heads, mx)

        h = xc[j].astype(F32) + dot(o_s[...].T, wo[...]) + wide(bo_ref[...])
        n = layer_norm(h, wide(g2_ref[...]), wide(c2_ref[...])).astype(BF16)
        h = h + wide(b2_ref[...])
        fc = 1024
        for c in range(d_ff // fc):
            u = dot(n, w1[:, c * fc : (c + 1) * fc]) + wide(b1_ref[c * fc : (c + 1) * fc])
            u = (0.5 * u * (1.0 + lax.erf(u * math.sqrt(0.5)))).astype(BF16)
            h = h + dot(u, w2[c * fc : (c + 1) * fc, :])
        y = layer_norm(h, wide(gp_ref[...]), wide(cp_ref[...])).astype(BF16)

        @pl.when(j >= 2)
        def _():
            for kind, dev in enumerate((near, across_x, across_y)):
                own(j - 2, kind, dev).wait_send()
            store_own(j - 2).wait()

        y_s[j % 2] = y
        for kind, dev in ((1, across_x), (2, across_y), (0, near)):
            own(j, kind, dev).start()
        store_own(j).start()

        @pl.when(j >= 1)
        def _():
            relay_first(j - 1)

        @pl.when(j >= 2)
        def _():
            relay_second(j - 2)

        return carry

    lax.fori_loop(0, n_dev, step, 0)

    last = n_dev - 1
    relay_first(last)
    relay_second(last - 1)
    relay_second(last)
    for j in (last - 1, last):
        for kind, dev in enumerate((near, across_x, across_y)):
            own(j, kind, dev).wait_send()
        store_own(j).wait()

    def drain(j, carry):
        for t in (1, 3, 5, 7):
            arrived(flip(t), j)
        forward(across_x, j, near, 0).wait_send()
        forward(across_y, j, near, 1).wait_send()
        forward(across_x, j, across_y, 2).wait_send()
        forward(diag, j, near, 3).wait_send()
        return carry

    lax.fori_loop(0, n_dev, drain, 0)
    for t in range(1, n_dev):
        x_copy(flip(t), t).wait_send()


def cache_kernel(y_ref, wk_ref, wv_ref, bv_ref, k_ref, v_ref, wt, bias):
    layers, _, cols = wk_ref.shape
    half = layers * cols

    @pl.when((pl.program_id(0) == 0) & (pl.program_id(1) == 0))
    def _():
        for i in range(layers):
            wt[i * cols : (i + 1) * cols, :] = wk_ref[i].T
            wt[half + i * cols : half + (i + 1) * cols, :] = wv_ref[i].T
            bias[i * cols : (i + 1) * cols, :] = jnp.broadcast_to(bv_ref[i : i + 1, :].astype(F32), (cols, cols)).T

    out = dot(wt[...], y_ref[0], 1, 1)
    for i in range(layers):
        k_ref[i, 0] = out[i * cols : (i + 1) * cols].astype(BF16)
        v = out[half + i * cols : half + (i + 1) * cols] + bias[i * cols : (i + 1) * cols, :1]
        v_ref[i, 0] = v.astype(BF16)


def solution(mesh):
    n_dev = mesh.shape["sp"]

    def device_fn(x, ln1_gain, ln1_bias, w_query, b_query, w_key, w_value, b_value, w_out, b_out, ln2_gain, ln2_bias, w_up, b_up, w_down, b_down, lnp_gain, lnp_bias, cross_wk, cross_wv, cross_bv):
        clips, rows, d_model = x.shape
        d_ff = w_up.shape[1]
        frames = rows * n_dev
        layers, _, cols = cross_wk.shape
        pairs = d_model // 128
        row = lambda a: a
        hbm = pl.BlockSpec(memory_space=pl.ANY)
        vmem = pl.BlockSpec(memory_space=pltpu.VMEM)
        dma = pltpu.SemaphoreType.DMA
        y_all = pl.pallas_call(
            functools.partial(encoder_kernel, n_dev=n_dev, rows=rows),
            out_shape=jax.ShapeDtypeStruct((clips, frames, d_model), BF16),
            in_specs=[hbm] * 7 + [vmem] * 11,
            out_specs=hbm,
            scratch_shapes=[
                pltpu.VMEM((n_dev, rows, d_model), BF16),
                pltpu.VMEM((d_model, d_model), BF16),
                pltpu.VMEM((d_model, d_model), BF16),
                pltpu.VMEM((d_model, d_model), BF16),
                pltpu.VMEM((d_model, d_model), BF16),
                pltpu.VMEM((d_model, d_ff), BF16),
                pltpu.VMEM((d_ff, d_model), BF16),
                pltpu.VMEM((pairs, frames, 128), BF16),
                pltpu.VMEM((pairs, frames, 128), BF16),
                pltpu.VMEM((2 * pairs, V_ROWS, frames), BF16),
                pltpu.VMEM((frames, rows), F32),
                pltpu.VMEM((frames, rows), F32),
                pltpu.VMEM((d_model, rows), BF16),
                pltpu.VMEM((2, rows, d_model), BF16),
                dma((n_dev,)),
                dma((n_dev,)),
                dma((3, 2)),
                dma((4, n_dev)),
                dma((n_dev, n_dev)),
                dma((7,)),
                dma((2,)),
            ],
            compiler_params=pltpu.CompilerParams(
                collective_id=0, has_side_effects=True, vmem_limit_bytes=67043328
            ),
            name="encoder",
        )(
            x, w_query, w_key, w_value, w_out, w_up, w_down,
            row(ln1_gain), row(ln1_bias), row(b_query), row(b_value), row(b_out), row(ln2_gain), row(ln2_bias),
            row(b_up), row(b_down), row(lnp_gain), row(lnp_bias),
        )
        fb = 512
        shape = (layers, clips, cols, frames)
        spec = pl.BlockSpec((layers, 1, cols, fb), lambda b, f: (0, b, 0, f))
        k, v = pl.pallas_call(
            cache_kernel,
            grid=(clips, frames // fb),
            out_shape=[jax.ShapeDtypeStruct(shape, BF16)] * 2,
            in_specs=[
                pl.BlockSpec((1, fb, d_model), lambda b, f: (b, f, 0)),
                pl.BlockSpec((layers, d_model, cols), lambda b, f: (0, 0, 0)),
                pl.BlockSpec((layers, d_model, cols), lambda b, f: (0, 0, 0)),
                pl.BlockSpec((layers, cols), lambda b, f: (0, 0)),
            ],
            out_specs=[spec, spec],
            scratch_shapes=[pltpu.VMEM((2 * layers * cols, d_model), BF16), pltpu.VMEM((layers * cols, cols), F32)],
            name="caches",
        )(y_all, cross_wk, cross_wv, cross_bv)
        heads = lambda a: a.reshape(layers, clips, cols // HEAD_DIM, HEAD_DIM, frames).transpose(0, 1, 4, 2, 3)
        return heads(k), heads(v)

    in_specs = (P("dp", "sp", None),) + (P(),) * 17 + (P(None, None, "sp"), P(None, None, "sp"), P(None, "sp"))
    out_specs = (P(None, "dp", None, "sp", None), P(None, "dp", None, "sp", None))
    return jax.shard_map(device_fn, mesh=mesh, in_specs=in_specs, out_specs=out_specs, check_vma=False)
```

```python
import functools
import math

import jax
import jax.numpy as jnp
from jax import lax
from jax.experimental import pallas as pl
from jax.experimental.pallas import tpu as pltpu
from jax.sharding import PartitionSpec as P

HEAD_DIM = 64
LN_EPS = 1e-5
LOG2E = math.log2(math.e)
V_ROWS = 80
F32 = jnp.float32
BF16 = jnp.bfloat16


def layer_norm(h, gain, bias):
    mean = jnp.mean(h, axis=-1, keepdims=True)
    centered = h - mean
    var = jnp.mean(centered * centered, axis=-1, keepdims=True)
    return centered * lax.rsqrt(var + LN_EPS) * gain + bias


def wide(row):
    return row.astype(F32).reshape(1, -1)


def dot(a, b, ca=1, cb=0):
    return lax.dot_general(a, b, (((ca,), (cb,)), ((), ())), preferred_element_type=F32)


def encoder_kernel(
    x_hbm, wq_hbm, wk_hbm, wv_hbm, wo_hbm, w1_hbm, w2_hbm,
    g1_ref, c1_ref, bq_ref, bv_ref, bo_ref, g2_ref, c2_ref, b1_ref, b2_ref, gp_ref, cp_ref,
    y_hbm,
    xc, wq, wk, wv, wo, w1, w2, q_s, k_s, v_s, sa, sb, mx_s, o_s, y_s,
    x_send, x_recv, kv_send, kv_recv, credit, y_send, f_send, y_recv, load_sem, y_loc,
    *, n_dev, rows,
):
    d_model = wq.shape[0]
    d_ff = w1.shape[1]
    pairs = d_model // 128
    frames = n_dev * rows
    scale = HEAD_DIM**-0.25
    me = lax.axis_index("sp")
    core = me % 2
    px = (me // 2) % 2
    py = me // 4

    def flip(t):
        c = core + (t % 2) * (1 - 2 * core)
        x = px + ((t // 2) % 2) * (1 - 2 * px)
        y = py + (t // 4) * (1 - 2 * py)
        return y * 4 + x * 2 + c

    near, across_x, across_y, diag = flip(1), flip(2), flip(4), flip(6)

    barrier = pltpu.get_barrier_semaphore()
    for dev in (near, across_x, across_y, diag):
        pl.semaphore_signal(barrier, inc=1, device_id={"sp": dev}, device_id_type=pl.DeviceIdType.MESH)
    pl.semaphore_wait(barrier, 4)

    chips = n_dev // 2
    chip = me // 2

    def x_copy(w, t):
        dev = flip(2 * t)
        return pltpu.make_async_remote_copy(
            src_ref=x_hbm.at[w * chips + dev // 2], dst_ref=xc.at[w, chip],
            send_sem=x_send.at[w, t], recv_sem=x_recv.at[w, chip],
            device_id={"sp": dev}, device_id_type=pl.DeviceIdType.MESH,
        )

    def x_arrival(w, slot):
        return pltpu.make_async_remote_copy(
            src_ref=x_hbm.at[0], dst_ref=xc.at[w, slot], send_sem=x_send.at[w, 0], recv_sem=x_recv.at[w, slot],
            device_id={"sp": near}, device_id_type=pl.DeviceIdType.MESH,
        )

    own_x = [pltpu.make_async_copy(x_hbm.at[w * chips + chip], xc.at[w, chip], load_sem.at[6 + w]) for w in (0, 1)]
    own_x[0].start()
    for t in (1, 2, 3):
        x_copy(0, t).start()
    loads = [
        pltpu.make_async_copy(a, b, load_sem.at[i])
        for i, (a, b) in enumerate(
            ((wq_hbm, wq), (wk_hbm, wk), (wv_hbm, wv), (wo_hbm, wo), (w1_hbm, w1), (w2_hbm, w2))
        )
    ]
    for c in loads:
        c.start()
    own_x[1].start()

    ones = (lax.broadcasted_iota(jnp.int32, (V_ROWS - HEAD_DIM, frames), 0) == 0).astype(BF16)
    for h in range(2 * pairs):
        v_s[h, HEAD_DIM:, :] = ones

    for c in (*own_x, *loads[:3]):
        c.wait()

    def kv_copies(s):
        at = pl.ds(pl.multiple_of((core * chips + s) * rows, rows), rows)
        return [
            pltpu.make_async_remote_copy(
                src_ref=ref, dst_ref=ref, send_sem=kv_send.at[i, s], recv_sem=kv_recv.at[i, s],
                device_id={"sp": near}, device_id_type=pl.DeviceIdType.MESH,
            )
            for i, ref in enumerate((k_s.at[:, at, :], v_s.at[:, pl.ds(0, HEAD_DIM), at]))
        ]

    def project(w, t):
        slot = flip(2 * t) // 2

        @pl.when(t > 0)
        def _():
            x_arrival(w, slot).wait_recv()

        a = layer_norm(xc[w, slot].astype(F32), wide(g1_ref[...]), wide(c1_ref[...])).astype(BF16)
        at_q = pl.multiple_of(slot * rows, rows)
        at = pl.multiple_of((core * chips + slot) * rows, rows)
        q = ((dot(a, wq[...]) + wide(bq_ref[...])) * scale).astype(BF16)
        k = (dot(a, wk[...]) * scale).astype(BF16)
        for p in range(pairs):
            q_s[p, pl.ds(at_q, rows), :] = q[:, p * 128 : (p + 1) * 128]
            k_s[p, pl.ds(at, rows), :] = k[:, p * 128 : (p + 1) * 128]
        v = (dot(a, wv[...]) + wide(bv_ref[...])).astype(BF16).T
        for h in range(2 * pairs):
            v_s[h, :HEAD_DIM, pl.ds(at, rows)] = v[h * HEAD_DIM : (h + 1) * HEAD_DIM]

        @pl.when((w == 1) & (t == 0))
        def _():
            pl.semaphore_wait(credit, 1)

        for c in kv_copies(slot):
            c.start()

    lane = lax.broadcasted_iota(jnp.int32, (rows, 128), 1)
    kc = 256

    def y_block(src, j):
        clip = (j // chips) * chips + src // 2
        return y_hbm.at[clip, pl.ds(pl.multiple_of((2 * (j % chips) + src % 2) * rows, rows), rows)]

    def y_copy(src_ref, src, j, dst_dev, sem):
        return pltpu.make_async_remote_copy(
            src_ref=src_ref, dst_ref=y_block(src, j),
            send_sem=sem, recv_sem=y_recv.at[src, j],
            device_id={"sp": dst_dev}, device_id_type=pl.DeviceIdType.MESH,
        )

    def forward(src, j, dst_dev, kind):
        return y_copy(y_block(src, j), src, j, dst_dev, f_send.at[kind, j])

    def arrived(src, j):
        y_copy(y_block(src, j), src, j, near, f_send.at[0, j]).wait_recv()

    def own(j, kind, dst_dev):
        return y_copy(y_s.at[j % 2], me, j, dst_dev, y_send.at[kind, j % 2])

    def store_own(j):
        return pltpu.make_async_copy(y_s.at[j % 2], y_block(me, j), y_loc.at[j % 2])

    def relay_first(j):
        arrived(across_x, j)
        arrived(across_y, j)
        forward(across_x, j, near, 0).start()
        forward(across_y, j, near, 1).start()
        via, to = (1 - core) * across_x + core * across_y, (1 - core) * across_y + core * across_x
        forward(via, j, to, 2).start()

    def relay_second(j):
        arrived(diag, j)
        forward(diag, j, near, 3).start()

    def score_chunk(pair, q, s_ref, half, c, mx):
        at = slice(c * kc, (c + 1) * kc)
        x = dot(k_s[pair, at, :], q, 1, 1)
        s_ref[half, at, :] = x
        return jnp.maximum(mx, jnp.max(x.reshape(kc // 8, 8, rows), axis=0))

    def split_pair(pair, s):
        q = q_s[pair, pl.ds(pl.multiple_of(s * rows, rows), rows), :]
        return [jnp.where(keep, q, jnp.zeros_like(q)) for keep in (lane < HEAD_DIM, lane >= HEAD_DIM)]

    mx0 = jnp.full((8, rows), -jnp.inf, F32)

    def first_scores():
        q = split_pair(0, 0)
        for half in (0, 1):
            mx = mx0
            for c in range(frames // kc):
                mx = score_chunk(0, q[half], sa, half, c, mx)
            mx_s[0, half] = mx

    def attend(pair, cur, cur_mx, next_pair, next_s, nxt, nxt_mx):
        top = [jnp.max(mx_s[cur_mx, half], axis=0, keepdims=True) * LOG2E for half in (0, 1)]
        q = split_pair(next_pair, next_s)
        mx = [mx0, mx0]
        o = [jnp.zeros((V_ROWS, rows), F32)] * 2
        for c in range(frames // kc):
            at = slice(c * kc, (c + 1) * kc)
            for half in (0, 1):
                mx[half] = score_chunk(next_pair, q[half], nxt, half, c, mx[half])
                p = jnp.exp2(cur[half, at, :] * LOG2E - top[half]).astype(BF16)
                o[half] = o[half] + dot(v_s[2 * pair + half, :, at], p)
        for half in (0, 1):
            mx_s[nxt_mx, half] = mx[half]
            out = (o[half][:HEAD_DIM] * (1.0 / o[half][HEAD_DIM : HEAD_DIM + 1])).astype(BF16)
            o_s[pl.ds(pl.multiple_of(pair * 128 + half * HEAD_DIM, HEAD_DIM), HEAD_DIM), :] = out

    def step(w, s):
        j = w * chips + s

        def two_pairs(i, carry):
            pair = 2 * i
            wrap = (pair + 2) // pairs

            @pl.when(i >= 0)
            def _():
                attend(pair, sa, 0, pair + 1, s, sb, 1)

            @pl.when(i < pairs)
            def _():
                attend(pair + 1, sb, 1, (pair + 2) % pairs, jnp.minimum(s + wrap, chips - 1), sa, 0)

            return carry

        lax.fori_loop(0, pairs // 2, two_pairs, 0)

        h = xc[w, s].astype(F32) + dot(o_s[...].T, wo[...]) + wide(bo_ref[...])
        n = layer_norm(h, wide(g2_ref[...]), wide(c2_ref[...])).astype(BF16)
        h = h + wide(b2_ref[...])
        fc = 1024
        for c in range(d_ff // fc):
            u = dot(n, w1[:, c * fc : (c + 1) * fc]) + wide(b1_ref[c * fc : (c + 1) * fc])
            u = (0.5 * u * (1.0 + lax.erf(u * math.sqrt(0.5)))).astype(BF16)
            h = h + dot(u, w2[c * fc : (c + 1) * fc, :])
        y = layer_norm(h, wide(gp_ref[...]), wide(cp_ref[...])).astype(BF16)

        @pl.when(j >= 2)
        def _():
            for kind, dev in enumerate((near, across_x, across_y)):
                own(j - 2, kind, dev).wait_send()
            store_own(j - 2).wait()

        y_s[j % 2] = y
        for kind, dev in ((1, across_x), (2, across_y), (0, near)):
            own(j, kind, dev).start()
        store_own(j).start()

        @pl.when(j >= 1)
        def _():
            relay_first(j - 1)

        @pl.when(j >= 2)
        def _():
            relay_second(j - 2)

    def wave(w, carry):
        lax.fori_loop(0, chips, lambda t, c: (project(w, t), c)[1], 0)

        @pl.when(w == 0)
        def _():
            for t in (1, 2, 3):
                x_copy(1, t).start()
            for c in loads[3:]:
                c.wait()

        for s in range(chips):
            for c in kv_copies(s):
                c.wait()
        first_scores()
        lax.fori_loop(0, chips, lambda s, c: (step(w, s), c)[1], 0)

        @pl.when(w == 0)
        def _():
            pl.semaphore_signal(credit, inc=1, device_id={"sp": near}, device_id_type=pl.DeviceIdType.MESH)

        return carry

    lax.fori_loop(0, 2, wave, 0)

    last = n_dev - 1
    relay_first(last)
    relay_second(last - 1)
    relay_second(last)
    for j in (last - 1, last):
        for kind, dev in enumerate((near, across_x, across_y)):
            own(j, kind, dev).wait_send()
        store_own(j).wait()

    def drain(j, carry):
        for t in (1, 3, 5, 7):
            arrived(flip(t), j)
        forward(across_x, j, near, 0).wait_send()
        forward(across_y, j, near, 1).wait_send()
        forward(across_x, j, across_y, 2).wait_send()
        forward(diag, j, near, 3).wait_send()
        return carry

    lax.fori_loop(0, n_dev, drain, 0)
    for w in (0, 1):
        for t in (1, 2, 3):
            x_copy(w, t).wait_send()


def cache_kernel(y_ref, wk_ref, wv_ref, bv_ref, k_ref, v_ref, wt, bias):
    layers, _, cols = wk_ref.shape
    half = layers * cols

    @pl.when((pl.program_id(0) == 0) & (pl.program_id(1) == 0))
    def _():
        for i in range(layers):
            wt[i * cols : (i + 1) * cols, :] = wk_ref[i].T
            wt[half + i * cols : half + (i + 1) * cols, :] = wv_ref[i].T
            bias[i * cols : (i + 1) * cols, :] = jnp.broadcast_to(bv_ref[i : i + 1, :].astype(F32), (cols, cols)).T

    out = dot(wt[...], y_ref[0], 1, 1)
    for i in range(layers):
        k_ref[i, 0] = out[i * cols : (i + 1) * cols].astype(BF16)
        v = out[half + i * cols : half + (i + 1) * cols] + bias[i * cols : (i + 1) * cols, :1]
        v_ref[i, 0] = v.astype(BF16)


def solution(mesh):
    n_dev = mesh.shape["sp"]

    def device_fn(x, ln1_gain, ln1_bias, w_query, b_query, w_key, w_value, b_value, w_out, b_out, ln2_gain, ln2_bias, w_up, b_up, w_down, b_down, lnp_gain, lnp_bias, cross_wk, cross_wv, cross_bv):
        clips, rows, d_model = x.shape
        d_ff = w_up.shape[1]
        frames = rows * n_dev
        layers, _, cols = cross_wk.shape
        pairs = d_model // 128
        row = lambda a: a
        hbm = pl.BlockSpec(memory_space=pl.ANY)
        vmem = pl.BlockSpec(memory_space=pltpu.VMEM)
        dma = pltpu.SemaphoreType.DMA
        y_all = pl.pallas_call(
            functools.partial(encoder_kernel, n_dev=n_dev, rows=rows),
            out_shape=jax.ShapeDtypeStruct((clips, frames, d_model), BF16),
            in_specs=[hbm] * 7 + [vmem] * 11,
            out_specs=hbm,
            scratch_shapes=[
                pltpu.VMEM((2, n_dev // 2, rows, d_model), BF16),
                pltpu.VMEM((d_model, d_model), BF16),
                pltpu.VMEM((d_model, d_model), BF16),
                pltpu.VMEM((d_model, d_model), BF16),
                pltpu.VMEM((d_model, d_model), BF16),
                pltpu.VMEM((d_model, d_ff), BF16),
                pltpu.VMEM((d_ff, d_model), BF16),
                pltpu.VMEM((pairs, frames // 2, 128), BF16),
                pltpu.VMEM((pairs, frames, 128), BF16),
                pltpu.VMEM((2 * pairs, V_ROWS, frames), BF16),
                pltpu.VMEM((2, frames, rows), F32),
                pltpu.VMEM((2, frames, rows), F32),
                pltpu.VMEM((2, 2, 8, rows), F32),
                pltpu.VMEM((d_model, rows), BF16),
                pltpu.VMEM((2, rows, d_model), BF16),
                dma((2, n_dev // 2)),
                dma((2, n_dev // 2)),
                dma((2, n_dev // 2)),
                dma((2, n_dev // 2)),
                pltpu.SemaphoreType.REGULAR,
                dma((3, 2)),
                dma((4, n_dev)),
                dma((n_dev, n_dev)),
                dma((8,)),
                dma((2,)),
            ],
            compiler_params=pltpu.CompilerParams(
                collective_id=0, has_side_effects=True, vmem_limit_bytes=67043328
            ),
            name="encoder",
        )(
            x, w_query, w_key, w_value, w_out, w_up, w_down,
            row(ln1_gain), row(ln1_bias), row(b_query), row(b_value), row(b_out), row(ln2_gain), row(ln2_bias),
            row(b_up), row(b_down), row(lnp_gain), row(lnp_bias),
        )
        fb = frames
        shape = (layers, clips, cols, frames)
        spec = pl.BlockSpec((layers, 1, cols, fb), lambda b, f: (0, b, 0, f))
        k, v = pl.pallas_call(
            cache_kernel,
            grid=(clips, frames // fb),
            out_shape=[jax.ShapeDtypeStruct(shape, BF16)] * 2,
            in_specs=[
                pl.BlockSpec((1, fb, d_model), lambda b, f: (b, f, 0)),
                pl.BlockSpec((layers, d_model, cols), lambda b, f: (0, 0, 0)),
                pl.BlockSpec((layers, d_model, cols), lambda b, f: (0, 0, 0)),
                pl.BlockSpec((layers, cols), lambda b, f: (0, 0)),
            ],
            out_specs=[spec, spec],
            scratch_shapes=[pltpu.VMEM((2 * layers * cols, d_model), BF16), pltpu.VMEM((layers * cols, cols), F32)],
            compiler_params=pltpu.CompilerParams(vmem_limit_bytes=67043328),
            name="caches",
        )(y_all, cross_wk, cross_wv, cross_bv)
        heads = lambda a: a.reshape(layers, clips, cols // HEAD_DIM, HEAD_DIM, frames).transpose(0, 1, 4, 2, 3)
        return heads(k), heads(v)

    in_specs = (P("dp", "sp", None),) + (P(),) * 17 + (P(None, None, "sp"), P(None, None, "sp"), P(None, "sp"))
    out_specs = (P(None, "dp", None, "sp", None), P(None, "dp", None, "sp", None))
    return jax.shard_map(device_fn, mesh=mesh, in_specs=in_specs, out_specs=out_specs, check_vma=False)
```

```python
import functools
import math

import jax
import jax.numpy as jnp
from jax import lax
from jax.experimental import pallas as pl
from jax.experimental.pallas import tpu as pltpu
from jax.sharding import PartitionSpec as P

HEAD_DIM = 64
LN_EPS = 1e-5
LOG2E = math.log2(math.e)
V_ROWS = 80
F32 = jnp.float32
BF16 = jnp.bfloat16


def layer_norm(h, gain, bias):
    mean = jnp.mean(h, axis=-1, keepdims=True)
    centered = h - mean
    var = jnp.mean(centered * centered, axis=-1, keepdims=True)
    return centered * lax.rsqrt(var + LN_EPS) * gain + bias


def wide(row):
    return row.astype(F32).reshape(1, -1)


def dot(a, b, ca=1, cb=0):
    return lax.dot_general(a, b, (((ca,), (cb,)), ((), ())), preferred_element_type=F32)


def cache_weights(wk_ref, wv_ref, bv_ref, wt, bias):
    layers, _, cols = wk_ref.shape
    for i in range(layers):
        wt[i * cols : (i + 1) * cols, :] = wk_ref[i].T
        wt[(layers + i) * cols : (layers + i + 1) * cols, :] = wv_ref[i].T
        bias[i * cols : (i + 1) * cols, :] = jnp.broadcast_to(bv_ref[i : i + 1, :].astype(F32), (cols, cols)).T


def cache_rows(y, wt, bias):
    half = bias.shape[0]
    out = dot(wt[...], y, 1, 1)
    return out[:half].astype(BF16), (out[half:] + bias[:, :1]).astype(BF16)


def encoder_kernel(
    x_hbm, wq_hbm, wk_hbm, wv_hbm, wo_hbm, w1_hbm, w2_hbm, ck_hbm, cv_hbm,
    g1_ref, c1_ref, bq_ref, bv_ref, bo_ref, g2_ref, c2_ref, b1_ref, b2_ref, gp_ref, cp_ref, cb_ref,
    y_hbm, kp_hbm, vp_hbm,
    xc, wq, wk, wv, wo, w1, w2, q_s, k_s, v_s, sa, sb, mx_s, o_s, y_s, ck_s, cv_s, wt_s, bias_s, cy_s, co_s,
    x_send, x_recv, kv_send, kv_recv, credit, y_send, f_send, y_recv, load_sem, y_loc, c_load, c_store,
    *, n_dev, rows,
):
    d_model = wq.shape[0]
    d_ff = w1.shape[1]
    pairs = d_model // 128
    frames = n_dev * rows
    scale = HEAD_DIM**-0.25
    me = lax.axis_index("sp")
    core = me % 2
    px = (me // 2) % 2
    py = me // 4

    def flip(t):
        c = core + (t % 2) * (1 - 2 * core)
        x = px + ((t // 2) % 2) * (1 - 2 * px)
        y = py + (t // 4) * (1 - 2 * py)
        return y * 4 + x * 2 + c

    near, across_x, across_y, diag = flip(1), flip(2), flip(4), flip(6)

    barrier = pltpu.get_barrier_semaphore()
    for dev in (near, across_x, across_y, diag):
        pl.semaphore_signal(barrier, inc=1, device_id={"sp": dev}, device_id_type=pl.DeviceIdType.MESH)
    pl.semaphore_wait(barrier, 4)

    chips = n_dev // 2
    chip = me // 2

    def x_copy(w, t):
        dev = flip(2 * t)
        return pltpu.make_async_remote_copy(
            src_ref=x_hbm.at[w * chips + dev // 2], dst_ref=xc.at[w, chip],
            send_sem=x_send.at[w, t], recv_sem=x_recv.at[w, chip],
            device_id={"sp": dev}, device_id_type=pl.DeviceIdType.MESH,
        )

    def x_arrival(w, slot):
        return pltpu.make_async_remote_copy(
            src_ref=x_hbm.at[0], dst_ref=xc.at[w, slot], send_sem=x_send.at[w, 0], recv_sem=x_recv.at[w, slot],
            device_id={"sp": near}, device_id_type=pl.DeviceIdType.MESH,
        )

    own_x = [pltpu.make_async_copy(x_hbm.at[w * chips + chip], xc.at[w, chip], load_sem.at[8 + w]) for w in (0, 1)]
    own_x[0].start()
    for t in (1, 2, 3):
        x_copy(0, t).start()
    loads = [
        pltpu.make_async_copy(a, b, load_sem.at[i])
        for i, (a, b) in enumerate(
            ((wq_hbm, wq), (wk_hbm, wk), (wv_hbm, wv), (wo_hbm, wo), (w1_hbm, w1), (w2_hbm, w2), (ck_hbm, ck_s), (cv_hbm, cv_s))
        )
    ]
    for c in loads:
        c.start()
    own_x[1].start()

    ones = (lax.broadcasted_iota(jnp.int32, (V_ROWS - HEAD_DIM, frames), 0) == 0).astype(BF16)
    q_zero = jnp.zeros((HEAD_DIM, chips * rows), BF16)
    for h in range(2 * pairs):
        v_s[h, HEAD_DIM:, :] = ones
        q_s[h, HEAD_DIM * (1 - h % 2) : HEAD_DIM * (2 - h % 2), :] = q_zero

    for c in (*own_x, *loads[:3], *loads[6:]):
        c.wait()
    cache_weights(ck_s, cv_s, cb_ref, wt_s, bias_s)

    def kv_copies(s):
        at = pl.ds(pl.multiple_of((core * chips + s) * rows, rows), rows)
        return [
            pltpu.make_async_remote_copy(
                src_ref=ref, dst_ref=ref, send_sem=kv_send.at[i, s], recv_sem=kv_recv.at[i, s],
                device_id={"sp": near}, device_id_type=pl.DeviceIdType.MESH,
            )
            for i, ref in enumerate((k_s.at[:, at, :], v_s.at[:, pl.ds(0, HEAD_DIM), at]))
        ]

    def project(w, t):
        slot = flip(2 * t) // 2

        @pl.when(t > 0)
        def _():
            x_arrival(w, slot).wait_recv()

        @pl.when((w == 0) & (t == chips - 1))
        def _():
            for i in (1, 2, 3):
                x_copy(1, i).start()

        a = layer_norm(xc[w, slot].astype(F32), wide(g1_ref[...]), wide(c1_ref[...])).astype(BF16)
        at_q = pl.multiple_of(slot * rows, rows)
        at = pl.multiple_of((core * chips + slot) * rows, rows)
        q = ((dot(a, wq[...]) + wide(bq_ref[...])) * scale).astype(BF16).T
        k = (dot(a, wk[...]) * scale).astype(BF16)
        for p in range(pairs):
            for half in (0, 1):
                h = 2 * p + half
                own_rows = slice(half * HEAD_DIM, (half + 1) * HEAD_DIM)
                q_s[h, own_rows, pl.ds(at_q, rows)] = q[h * HEAD_DIM : (h + 1) * HEAD_DIM]
            k_s[p, pl.ds(at, rows), :] = k[:, p * 128 : (p + 1) * 128]
        v = (dot(a, wv[...]) + wide(bv_ref[...])).astype(BF16).T
        for h in range(2 * pairs):
            v_s[h, :HEAD_DIM, pl.ds(at, rows)] = v[h * HEAD_DIM : (h + 1) * HEAD_DIM]

        @pl.when((w == 1) & (t == 0))
        def _():
            pl.semaphore_wait(credit, 1)

        for c in kv_copies(slot):
            c.start()

    kc = 256

    def y_block(src, j):
        clip = (j // chips) * chips + src // 2
        return y_hbm.at[clip, pl.ds(pl.multiple_of((2 * (j % chips) + src % 2) * rows, rows), rows)]

    def y_copy(src_ref, src, j, dst_dev, sem):
        return pltpu.make_async_remote_copy(
            src_ref=src_ref, dst_ref=y_block(src, j),
            send_sem=sem, recv_sem=y_recv.at[src, j],
            device_id={"sp": dst_dev}, device_id_type=pl.DeviceIdType.MESH,
        )

    def forward(src, j, dst_dev, kind):
        return y_copy(y_block(src, j), src, j, dst_dev, f_send.at[kind, j])

    def arrived(src, j):
        y_copy(y_block(src, j), src, j, near, f_send.at[0, j]).wait_recv()

    def own(j, kind, dst_dev):
        return y_copy(y_s.at[j % 2], me, j, dst_dev, y_send.at[kind, j % 2])

    def store_own(j):
        return pltpu.make_async_copy(y_s.at[j % 2], y_block(me, j), y_loc.at[j % 2])

    def relay_first(j):
        arrived(across_x, j)
        arrived(across_y, j)
        forward(across_x, j, near, 0).start()
        forward(across_y, j, near, 1).start()
        via, to = (1 - core) * across_x + core * across_y, (1 - core) * across_y + core * across_x
        forward(via, j, to, 2).start()

    def relay_second(j):
        arrived(diag, j)
        forward(diag, j, near, 3).start()

    def score_chunk(pair, q, s_ref, half, c, mx):
        at = slice(c * kc, (c + 1) * kc)
        x = dot(k_s[pair, at, :], q)
        s_ref[half, at, :] = x
        return jnp.maximum(mx, jnp.max(x.reshape(kc // 8, 8, rows), axis=0))

    def queries(pair, s):
        at = pl.ds(pl.multiple_of(s * rows, rows), rows)
        return [q_s[2 * pair + half, :, at] for half in (0, 1)]

    mx0 = jnp.full((8, rows), -jnp.inf, F32)

    def first_scores():
        q = queries(0, 0)
        for half in (0, 1):
            mx = mx0
            for c in range(frames // kc):
                mx = score_chunk(0, q[half], sa, half, c, mx)
            mx_s[0, half] = mx

    def attend(pair, cur, cur_mx, next_pair, next_s, nxt, nxt_mx):
        top = [jnp.max(mx_s[cur_mx, half], axis=0, keepdims=True) * LOG2E for half in (0, 1)]
        q = queries(next_pair, next_s)
        mx = [mx0, mx0]
        o = [jnp.zeros((V_ROWS, rows), F32)] * 2
        for c in range(frames // kc):
            at = slice(c * kc, (c + 1) * kc)
            for half in (0, 1):
                mx[half] = score_chunk(next_pair, q[half], nxt, half, c, mx[half])
                p = jnp.exp2(cur[half, at, :] * LOG2E - top[half]).astype(BF16)
                o[half] = o[half] + dot(v_s[2 * pair + half, :, at], p)
        for half in (0, 1):
            mx_s[nxt_mx, half] = mx[half]
            out = (o[half][:HEAD_DIM] * (1.0 / o[half][HEAD_DIM : HEAD_DIM + 1])).astype(BF16)
            o_s[pl.ds(pl.multiple_of(pair * 128 + half * HEAD_DIM, HEAD_DIM), HEAD_DIM), :] = out

    def step(w, s):
        j = w * chips + s

        def two_pairs(i, carry):
            pair = 2 * i
            wrap = (pair + 2) // pairs

            @pl.when(i >= 0)
            def _():
                attend(pair, sa, 0, pair + 1, s, sb, 1)

            @pl.when(i < pairs)
            def _():
                attend(pair + 1, sb, 1, (pair + 2) % pairs, jnp.minimum(s + wrap, chips - 1), sa, 0)

            return carry

        lax.fori_loop(0, pairs // 2, two_pairs, 0)

        @pl.when(j == chips)
        def _():
            relay_first(j - 1)

        h = xc[w, s].astype(F32) + dot(o_s[...].T, wo[...]) + wide(bo_ref[...])
        n = layer_norm(h, wide(g2_ref[...]), wide(c2_ref[...])).astype(BF16)
        h = h + wide(b2_ref[...])
        fc = 1024
        for c in range(d_ff // fc):
            u = dot(n, w1[:, c * fc : (c + 1) * fc]) + wide(b1_ref[c * fc : (c + 1) * fc])
            u = (0.5 * u * (1.0 + lax.erf(u * math.sqrt(0.5)))).astype(BF16)
            h = h + dot(u, w2[c * fc : (c + 1) * fc, :])
        y = layer_norm(h, wide(gp_ref[...]), wide(cp_ref[...])).astype(BF16)

        @pl.when(j >= 2)
        def _():
            for kind, dev in enumerate((near, across_x, across_y)):
                own(j - 2, kind, dev).wait_send()
            store_own(j - 2).wait()

        y_s[j % 2] = y
        for kind, dev in ((1, across_x), (2, across_y), (0, near)):
            own(j, kind, dev).start()
        store_own(j).start()

        @pl.when((j >= 1) & (j != chips))
        def _():
            relay_first(j - 1)

        @pl.when(j >= 3)
        def _():
            relay_second(j - 3)

    def wave(w, carry):
        lax.fori_loop(0, chips, lambda t, c: (project(w, t), c)[1], 0)

        @pl.when(w == 0)
        def _():
            for c in loads[3:6]:
                c.wait()

        for s in range(chips):
            for c in kv_copies(s):
                c.wait()
        first_scores()
        lax.fori_loop(0, chips, lambda s, c: (step(w, s), c)[1], 0)

        @pl.when(w == 0)
        def _():
            pl.semaphore_signal(credit, inc=1, device_id={"sp": near}, device_id_type=pl.DeviceIdType.MESH)

        return carry

    lax.fori_loop(0, 2, wave, 0)

    last = n_dev - 1
    ahead, chunk = cy_s.shape[:2]
    layers, _, cols = ck_s.shape

    def caches(count, where):
        def load(t):
            clip, at = where(t)
            at = pl.multiple_of(at * chunk, chunk)
            return pltpu.make_async_copy(y_hbm.at[clip, pl.ds(at, chunk)], cy_s.at[t % ahead], c_load.at[t % ahead])

        def stores(t):
            clip, at = where(t)
            at = pl.multiple_of(at * chunk, chunk)
            return [
                pltpu.make_async_copy(co_s.at[t % 2, i], dst.at[:, clip, :, pl.ds(at, chunk)], c_store.at[t % 2, i])
                for i, dst in enumerate((kp_hbm, vp_hbm))
            ]

        for t in range(ahead - 1):
            load(t).start()

        def task(t, carry):
            @pl.when(t + ahead - 1 < count)
            def _():
                load(t + ahead - 1).start()

            @pl.when(t >= 2)
            def _():
                for c in stores(t - 2):
                    c.wait()

            load(t).wait()
            for i, x in enumerate(cache_rows(cy_s[t % ahead], wt_s, bias_s)):
                for l in range(layers):
                    co_s[t % 2, i, l] = x[l * cols : (l + 1) * cols]
            for c in stores(t):
                c.start()
            return carry

        lax.fori_loop(0, count, task, 0)
        for t in (count - 2, count - 1):
            for c in stores(t):
                c.wait()

    def near_arrived(first, end):
        def wait(j, carry):
            for t in (1, 3, 5, 7):
                arrived(flip(t), j)
            return carry

        lax.fori_loop(first, end, wait, 0)

    def own_done(j):
        for kind, dev in enumerate((near, across_x, across_y)):
            own(j, kind, dev).wait_send()
        store_own(j).wait()

    relay_second(last - 2)
    near_arrived(0, chips)
    caches(chips * chips, lambda t: (t // chips, t % chips))
    relay_first(last)
    near_arrived(chips, last - 1)

    caches(2 * chips, lambda t: (chips + t // 2, t % 2))
    relay_second(last - 1)
    relay_second(last)
    own_done(last - 1)
    own_done(last)
    near_arrived(last - 1, n_dev)

    def drain(j, carry):
        forward(across_x, j, near, 0).wait_send()
        forward(across_y, j, near, 1).wait_send()
        forward(across_x, j, across_y, 2).wait_send()
        forward(diag, j, near, 3).wait_send()
        return carry

    lax.fori_loop(0, n_dev, drain, 0)
    for w in (0, 1):
        for t in (1, 2, 3):
            x_copy(w, t).wait_send()


def cache_kernel(
    kp_hbm, vp_hbm, y_hbm, wk_ref, wv_ref, bv_ref, k_hbm, v_hbm,
    wt, bias, y_s, kept_s, tail_s, new_s, y_sem, kept_sem, tail_sem, new_sem,
):
    layers, _, cols = wk_ref.shape
    chips, half, _ = y_s.shape
    frames = 2 * half
    y_in = [
        pltpu.make_async_copy(y_hbm.at[chips + i, pl.ds(half, half)], y_s.at[i], y_sem.at[i]) for i in range(chips)
    ]
    moves = []
    for i in range(chips):
        for n, (src, dst) in enumerate(((kp_hbm, k_hbm), (vp_hbm, v_hbm))):
            for buf, sem, clip, at in ((kept_s, kept_sem, i, pl.ds(0, frames)), (tail_s, tail_sem, chips + i, pl.ds(0, half))):
                moves.append((
                    pltpu.make_async_copy(src.at[:, clip, :, at], buf.at[i, n], sem.at[0, i, n]),
                    pltpu.make_async_copy(buf.at[i, n], dst.at[:, clip, :, at], sem.at[1, i, n]),
                ))
    new = [
        [
            pltpu.make_async_copy(new_s.at[i, n], dst.at[:, chips + i, :, pl.ds(half, half)], new_sem.at[i, n])
            for n, dst in enumerate((k_hbm, v_hbm))
        ]
        for i in range(chips)
    ]
    y_in[0].start()
    y_in[1].start()
    for load, _ in moves[:8]:
        load.start()
    y_in[2].start()
    y_in[3].start()
    for load, _ in moves[8:]:
        load.start()
    cache_weights(wk_ref, wv_ref, bv_ref, wt, bias)
    for i in range(chips):
        y_in[i].wait()
        for n, x in enumerate(cache_rows(y_s[i], wt, bias)):
            for l in range(layers):
                new_s[i, n, l] = x[l * cols : (l + 1) * cols]
        for c in new[i]:
            c.start()
        for load, store in moves[4 * i : 4 * i + 4]:
            load.wait()
            store.start()
    for _, store in moves:
        store.wait()
    for c in sum(new, []):
        c.wait()


def solution(mesh):
    n_dev = mesh.shape["sp"]

    def device_fn(x, ln1_gain, ln1_bias, w_query, b_query, w_key, w_value, b_value, w_out, b_out, ln2_gain, ln2_bias, w_up, b_up, w_down, b_down, lnp_gain, lnp_bias, cross_wk, cross_wv, cross_bv):
        clips, rows, d_model = x.shape
        d_ff = w_up.shape[1]
        frames = rows * n_dev
        layers, _, cols = cross_wk.shape
        pairs = d_model // 128
        row = lambda a: a
        hbm = pl.BlockSpec(memory_space=pl.ANY)
        vmem = pl.BlockSpec(memory_space=pltpu.VMEM)
        dma = pltpu.SemaphoreType.DMA
        shape = (layers, clips, cols, frames)
        chips = n_dev // 2
        chunk = 2 * rows
        y_all, k_part, v_part = pl.pallas_call(
            functools.partial(encoder_kernel, n_dev=n_dev, rows=rows),
            out_shape=[jax.ShapeDtypeStruct((clips, frames, d_model), BF16)] + [jax.ShapeDtypeStruct(shape, BF16)] * 2,
            in_specs=[hbm] * 9 + [vmem] * 12,
            out_specs=[hbm] * 3,
            scratch_shapes=[
                pltpu.VMEM((2, n_dev // 2, rows, d_model), BF16),
                pltpu.VMEM((d_model, d_model), BF16),
                pltpu.VMEM((d_model, d_model), BF16),
                pltpu.VMEM((d_model, d_model), BF16),
                pltpu.VMEM((d_model, d_model), BF16),
                pltpu.VMEM((d_model, d_ff), BF16),
                pltpu.VMEM((d_ff, d_model), BF16),
                pltpu.VMEM((2 * pairs, 128, frames // 2), BF16),
                pltpu.VMEM((pairs, frames, 128), BF16),
                pltpu.VMEM((2 * pairs, V_ROWS, frames), BF16),
                pltpu.VMEM((2, frames, rows), F32),
                pltpu.VMEM((2, frames, rows), F32),
                pltpu.VMEM((2, 2, 8, rows), F32),
                pltpu.VMEM((d_model, rows), BF16),
                pltpu.VMEM((2, rows, d_model), BF16),
                pltpu.VMEM((layers, d_model, cols), BF16),
                pltpu.VMEM((layers, d_model, cols), BF16),
                pltpu.VMEM((2 * layers * cols, d_model), BF16),
                pltpu.VMEM((layers * cols, cols), F32),
                pltpu.VMEM((4, chunk, d_model), BF16),
                pltpu.VMEM((2, 2, layers, cols, chunk), BF16),
                dma((2, n_dev // 2)),
                dma((2, n_dev // 2)),
                dma((2, n_dev // 2)),
                dma((2, n_dev // 2)),
                pltpu.SemaphoreType.REGULAR,
                dma((3, 2)),
                dma((4, n_dev)),
                dma((n_dev, n_dev)),
                dma((10,)),
                dma((2,)),
                dma((4,)),
                dma((2, 2)),
            ],
            compiler_params=pltpu.CompilerParams(
                collective_id=0, has_side_effects=True, vmem_limit_bytes=67043328
            ),
            name="encoder",
        )(
            x, w_query, w_key, w_value, w_out, w_up, w_down, cross_wk, cross_wv,
            row(ln1_gain), row(ln1_bias), row(b_query), row(b_value), row(b_out), row(ln2_gain), row(ln2_bias),
            row(b_up), row(b_down), row(lnp_gain), row(lnp_bias), cross_bv,
        )
        half = frames // 2
        k, v = pl.pallas_call(
            cache_kernel,
            out_shape=[jax.ShapeDtypeStruct(shape, BF16)] * 2,
            in_specs=[hbm] * 3 + [vmem] * 3,
            out_specs=[hbm] * 2,
            scratch_shapes=[
                pltpu.VMEM((2 * layers * cols, d_model), BF16),
                pltpu.VMEM((layers * cols, cols), F32),
                pltpu.VMEM((chips, half, d_model), BF16),
                pltpu.VMEM((chips, 2, layers, cols, frames), BF16),
                pltpu.VMEM((chips, 2, layers, cols, half), BF16),
                pltpu.VMEM((chips, 2, layers, cols, half), BF16),
                dma((chips,)),
                dma((2, chips, 2)),
                dma((2, chips, 2)),
                dma((chips, 2)),
            ],
            compiler_params=pltpu.CompilerParams(vmem_limit_bytes=67043328),
            name="caches",
        )(k_part, v_part, y_all, cross_wk, cross_wv, cross_bv)
        heads = lambda a: a.reshape(layers, clips, cols // HEAD_DIM, HEAD_DIM, frames).transpose(0, 1, 4, 2, 3)
        return heads(k), heads(v)

    in_specs = (P("dp", "sp", None),) + (P(),) * 17 + (P(None, None, "sp"), P(None, None, "sp"), P(None, "sp"))
    out_specs = (P(None, "dp", None, "sp", None), P(None, "dp", None, "sp", None))
    return jax.shard_map(device_fn, mesh=mesh, in_specs=in_specs, out_specs=out_specs, check_vma=False)
```

```python
import functools
import math

import jax
import jax.numpy as jnp
from jax import lax
from jax.experimental import pallas as pl
from jax.experimental.pallas import tpu as pltpu
from jax.sharding import PartitionSpec as P

HEAD_DIM = 64
LN_EPS = 1e-5
LOG2E = math.log2(math.e)
V_ROWS = 80
F32 = jnp.float32
BF16 = jnp.bfloat16


def layer_norm(h, gain, bias):
    mean = jnp.mean(h, axis=-1, keepdims=True)
    centered = h - mean
    var = jnp.mean(centered * centered, axis=-1, keepdims=True)
    return centered * lax.rsqrt(var + LN_EPS) * gain + bias


def wide(row):
    return row.astype(F32).reshape(1, -1)


def dot(a, b, ca=1, cb=0):
    return lax.dot_general(a, b, (((ca,), (cb,)), ((), ())), preferred_element_type=F32)


def cache_weights(wk_ref, wv_ref, bv_ref, wt, bias):
    layers, _, cols = wk_ref.shape
    for i in range(layers):
        wt[i * cols : (i + 1) * cols, :] = wk_ref[i].T
        wt[(layers + i) * cols : (layers + i + 1) * cols, :] = wv_ref[i].T
        bias[i * cols : (i + 1) * cols, :] = jnp.broadcast_to(bv_ref[i : i + 1, :].astype(F32), (cols, cols)).T


def cache_rows(y, wt, bias):
    half = bias.shape[0]
    out = dot(wt[...], y, 1, 1)
    return out[:half].astype(BF16), (out[half:] + bias[:, :1]).astype(BF16)


def encoder_kernel(
    x_hbm, wq_hbm, wk_hbm, wv_hbm, wo_hbm, w1_hbm, w2_hbm, ck_hbm, cv_hbm,
    g1_ref, c1_ref, bq_ref, bv_ref, bo_ref, g2_ref, c2_ref, b1_ref, b2_ref, gp_ref, cp_ref, cb_ref,
    y_hbm, kp_hbm, vp_hbm,
    xc, wq, wk, wv, wo, w1, w2, q_s, k_s, v_s, sa, sb, mx_s, o_s, y_s, ck_s, cv_s, wt_s, bias_s, cy_s, co_s,
    x_send, x_recv, kv_send, kv_recv, credit, y_send, f_send, y_recv, load_sem, y_loc, c_load, c_store,
    *, n_dev, rows,
):
    d_model = wq.shape[0]
    d_ff = w1.shape[1]
    pairs = d_model // 128
    frames = n_dev * rows
    scale = HEAD_DIM**-0.25
    me = lax.axis_index("sp")
    core = me % 2
    px = (me // 2) % 2
    py = me // 4

    def flip(t):
        c = core + (t % 2) * (1 - 2 * core)
        x = px + ((t // 2) % 2) * (1 - 2 * px)
        y = py + (t // 4) * (1 - 2 * py)
        return y * 4 + x * 2 + c

    near, across_x, across_y, diag = flip(1), flip(2), flip(4), flip(6)

    barrier = pltpu.get_barrier_semaphore()
    for dev in (near, across_x, across_y, diag):
        pl.semaphore_signal(barrier, inc=1, device_id={"sp": dev}, device_id_type=pl.DeviceIdType.MESH)
    pl.semaphore_wait(barrier, 4)

    chips = n_dev // 2
    chip = me // 2

    def x_copy(w, t):
        dev = flip(2 * t)
        return pltpu.make_async_remote_copy(
            src_ref=x_hbm.at[w * chips + dev // 2], dst_ref=xc.at[w, chip],
            send_sem=x_send.at[w, t], recv_sem=x_recv.at[w, chip],
            device_id={"sp": dev}, device_id_type=pl.DeviceIdType.MESH,
        )

    def x_arrival(w, slot):
        return pltpu.make_async_remote_copy(
            src_ref=x_hbm.at[0], dst_ref=xc.at[w, slot], send_sem=x_send.at[w, 0], recv_sem=x_recv.at[w, slot],
            device_id={"sp": near}, device_id_type=pl.DeviceIdType.MESH,
        )

    own_x = [pltpu.make_async_copy(x_hbm.at[w * chips + chip], xc.at[w, chip], load_sem.at[8 + w]) for w in (0, 1)]
    own_x[0].start()
    for t in (1, 2, 3):
        x_copy(0, t).start()
    loads = [
        pltpu.make_async_copy(a, b, load_sem.at[i])
        for i, (a, b) in enumerate(
            ((wq_hbm, wq), (wk_hbm, wk), (wv_hbm, wv), (wo_hbm, wo), (w1_hbm, w1), (w2_hbm, w2), (ck_hbm, ck_s), (cv_hbm, cv_s))
        )
    ]
    for c in loads:
        c.start()
    own_x[1].start()

    ones = (lax.broadcasted_iota(jnp.int32, (V_ROWS - HEAD_DIM, frames), 0) == 0).astype(BF16)
    q_zero = jnp.zeros((HEAD_DIM, chips * rows), BF16)
    for h in range(2 * pairs):
        v_s[h, HEAD_DIM:, :] = ones
        q_s[h, HEAD_DIM * (1 - h % 2) : HEAD_DIM * (2 - h % 2), :] = q_zero

    for c in (*own_x, *loads[:3], *loads[6:]):
        c.wait()
    cache_weights(ck_s, cv_s, cb_ref, wt_s, bias_s)

    def kv_copies(s):
        at = pl.ds(pl.multiple_of((core * chips + s) * rows, rows), rows)
        return [
            pltpu.make_async_remote_copy(
                src_ref=ref, dst_ref=ref, send_sem=kv_send.at[i, s], recv_sem=kv_recv.at[i, s],
                device_id={"sp": near}, device_id_type=pl.DeviceIdType.MESH,
            )
            for i, ref in enumerate((k_s.at[:, at, :], v_s.at[:, pl.ds(0, HEAD_DIM), at]))
        ]

    def project(w, t):
        slot = flip(2 * t) // 2

        @pl.when(t > 0)
        def _():
            x_arrival(w, slot).wait_recv()

        @pl.when((w == 0) & (t == chips - 1))
        def _():
            for i in (1, 2, 3):
                x_copy(1, i).start()

        a = layer_norm(xc[w, slot].astype(F32), wide(g1_ref[...]), wide(c1_ref[...])).astype(BF16)
        at_q = pl.multiple_of(slot * rows, rows)
        at = pl.multiple_of((core * chips + slot) * rows, rows)
        q = ((dot(a, wq[...]) + wide(bq_ref[...])) * scale).astype(BF16).T
        k = (dot(a, wk[...]) * scale).astype(BF16)
        for p in range(pairs):
            for half in (0, 1):
                h = 2 * p + half
                own_rows = slice(half * HEAD_DIM, (half + 1) * HEAD_DIM)
                q_s[h, own_rows, pl.ds(at_q, rows)] = q[h * HEAD_DIM : (h + 1) * HEAD_DIM]
            k_s[p, pl.ds(at, rows), :] = k[:, p * 128 : (p + 1) * 128]
        v = (dot(a, wv[...]) + wide(bv_ref[...])).astype(BF16).T
        for h in range(2 * pairs):
            v_s[h, :HEAD_DIM, pl.ds(at, rows)] = v[h * HEAD_DIM : (h + 1) * HEAD_DIM]

        @pl.when((w == 1) & (t == 0))
        def _():
            pl.semaphore_wait(credit, 1)

        for c in kv_copies(slot):
            c.start()

    kc = 256

    def y_block(src, j):
        clip = (j // chips) * chips + src // 2
        return y_hbm.at[clip, pl.ds(pl.multiple_of((2 * (j % chips) + src % 2) * rows, rows), rows)]

    def y_copy(src_ref, src, j, dst_dev, sem):
        return pltpu.make_async_remote_copy(
            src_ref=src_ref, dst_ref=y_block(src, j),
            send_sem=sem, recv_sem=y_recv.at[src, j],
            device_id={"sp": dst_dev}, device_id_type=pl.DeviceIdType.MESH,
        )

    def forward(src, j, dst_dev, kind):
        return y_copy(y_block(src, j), src, j, dst_dev, f_send.at[kind, j])

    def arrived(src, j):
        y_copy(y_block(src, j), src, j, near, f_send.at[0, j]).wait_recv()

    def own(j, kind, dst_dev):
        return y_copy(y_s.at[j % 2], me, j, dst_dev, y_send.at[kind, j % 2])

    def store_own(j):
        return pltpu.make_async_copy(y_s.at[j % 2], y_block(me, j), y_loc.at[j % 2])

    def relay_first(j):
        arrived(across_x, j)
        arrived(across_y, j)
        forward(across_x, j, near, 0).start()
        forward(across_y, j, near, 1).start()
        via, to = (1 - core) * across_x + core * across_y, (1 - core) * across_y + core * across_x
        forward(via, j, to, 2).start()

    def relay_second(j):
        arrived(diag, j)
        forward(diag, j, near, 3).start()

    def score_chunk(pair, q, s_ref, half, c, mx):
        at = slice(c * kc, (c + 1) * kc)
        x = dot(k_s[pair, at, :], q)
        s_ref[half, at, :] = x
        return jnp.maximum(mx, jnp.max(x.reshape(kc // 8, 8, rows), axis=0))

    def queries(pair, s):
        at = pl.ds(pl.multiple_of(s * rows, rows), rows)
        return [q_s[2 * pair + half, :, at] for half in (0, 1)]

    mx0 = jnp.full((8, rows), -jnp.inf, F32)

    def first_scores():
        q = queries(0, 0)
        for half in (0, 1):
            mx = mx0
            for c in range(frames // kc):
                mx = score_chunk(0, q[half], sa, half, c, mx)
            mx_s[0, half] = mx

    def attend(pair, cur, cur_mx, next_pair, next_s, nxt, nxt_mx):
        top = [jnp.max(mx_s[cur_mx, half], axis=0, keepdims=True) * LOG2E for half in (0, 1)]
        q = queries(next_pair, next_s)
        mx = [mx0, mx0]
        o = [jnp.zeros((V_ROWS, rows), F32)] * 2
        for c in range(frames // kc):
            at = slice(c * kc, (c + 1) * kc)
            for half in (0, 1):
                mx[half] = score_chunk(next_pair, q[half], nxt, half, c, mx[half])
                p = jnp.exp2(cur[half, at, :] * LOG2E - top[half]).astype(BF16)
                o[half] = o[half] + dot(v_s[2 * pair + half, :, at], p)
        for half in (0, 1):
            mx_s[nxt_mx, half] = mx[half]
            out = (o[half][:HEAD_DIM] * (1.0 / o[half][HEAD_DIM : HEAD_DIM + 1])).astype(BF16)
            o_s[pl.ds(pl.multiple_of(pair * 128 + half * HEAD_DIM, HEAD_DIM), HEAD_DIM), :] = out

    def step(w, s):
        j = w * chips + s

        def two_pairs(i, carry):
            pair = 2 * i
            wrap = (pair + 2) // pairs

            @pl.when(i >= 0)
            def _():
                attend(pair, sa, 0, pair + 1, s, sb, 1)

            @pl.when(i < pairs)
            def _():
                attend(pair + 1, sb, 1, (pair + 2) % pairs, jnp.minimum(s + wrap, chips - 1), sa, 0)

            return carry

        lax.fori_loop(0, pairs // 2, two_pairs, 0)

        @pl.when(j == chips)
        def _():
            relay_first(j - 1)

        h = xc[w, s].astype(F32) + dot(o_s[...].T, wo[...]) + wide(bo_ref[...])
        n = layer_norm(h, wide(g2_ref[...]), wide(c2_ref[...])).astype(BF16)
        h = h + wide(b2_ref[...])
        fc = 1024
        for c in range(d_ff // fc):
            u = dot(n, w1[:, c * fc : (c + 1) * fc]) + wide(b1_ref[c * fc : (c + 1) * fc])
            u = (0.5 * u * (1.0 + lax.erf(u * math.sqrt(0.5)))).astype(BF16)
            h = h + dot(u, w2[c * fc : (c + 1) * fc, :])
        y = layer_norm(h, wide(gp_ref[...]), wide(cp_ref[...])).astype(BF16)

        @pl.when(j >= 2)
        def _():
            for kind, dev in enumerate((near, across_x, across_y)):
                own(j - 2, kind, dev).wait_send()
            store_own(j - 2).wait()

        y_s[j % 2] = y
        for kind, dev in ((1, across_x), (2, across_y), (0, near)):
            own(j, kind, dev).start()
        store_own(j).start()

        @pl.when((j >= 1) & (j != chips))
        def _():
            relay_first(j - 1)

        @pl.when(j >= 3)
        def _():
            relay_second(j - 3)

    def wave(w, carry):
        lax.fori_loop(0, chips, lambda t, c: (project(w, t), c)[1], 0)

        @pl.when(w == 0)
        def _():
            for c in loads[3:6]:
                c.wait()

        for s in range(chips):
            for c in kv_copies(s):
                c.wait()
        first_scores()
        lax.fori_loop(0, chips, lambda s, c: (step(w, s), c)[1], 0)

        @pl.when(w == 0)
        def _():
            pl.semaphore_signal(credit, inc=1, device_id={"sp": near}, device_id_type=pl.DeviceIdType.MESH)

        return carry

    lax.fori_loop(0, 2, wave, 0)

    last = n_dev - 1
    ahead, chunk = cy_s.shape[:2]
    layers, _, cols = ck_s.shape

    def caches(count, where):
        def load(t):
            clip, at = where(t)
            at = pl.multiple_of(at * chunk, chunk)
            return pltpu.make_async_copy(y_hbm.at[clip, pl.ds(at, chunk)], cy_s.at[t % ahead], c_load.at[t % ahead])

        def stores(t):
            clip, at = where(t)
            at = pl.multiple_of(at * chunk, chunk)
            return [
                pltpu.make_async_copy(co_s.at[t % 2, i], dst.at[:, clip, :, pl.ds(at, chunk)], c_store.at[t % 2, i])
                for i, dst in enumerate((kp_hbm, vp_hbm))
            ]

        for t in range(ahead - 1):
            load(t).start()

        def task(t, carry):
            @pl.when(t + ahead - 1 < count)
            def _():
                load(t + ahead - 1).start()

            @pl.when(t >= 2)
            def _():
                for c in stores(t - 2):
                    c.wait()

            load(t).wait()
            for i, x in enumerate(cache_rows(cy_s[t % ahead], wt_s, bias_s)):
                for l in range(layers):
                    co_s[t % 2, i, l] = x[l * cols : (l + 1) * cols]
            for c in stores(t):
                c.start()
            return carry

        lax.fori_loop(0, count, task, 0)
        for t in (count - 2, count - 1):
            for c in stores(t):
                c.wait()

    def near_arrived(first, end):
        def wait(j, carry):
            for t in (1, 3, 5, 7):
                arrived(flip(t), j)
            return carry

        lax.fori_loop(first, end, wait, 0)

    def own_done(j):
        for kind, dev in enumerate((near, across_x, across_y)):
            own(j, kind, dev).wait_send()
        store_own(j).wait()

    relay_second(last - 2)
    near_arrived(0, chips)
    caches(10, lambda t: (t // chips, t % chips))
    relay_first(last)
    caches(6, lambda t: ((t + 10) // chips, (t + 10) % chips))

    relay_second(last - 1)
    relay_second(last)
    own_done(last - 1)
    own_done(last)
    near_arrived(chips, n_dev)

    def drain(j, carry):
        forward(across_x, j, near, 0).wait_send()
        forward(across_y, j, near, 1).wait_send()
        forward(across_x, j, across_y, 2).wait_send()
        forward(diag, j, near, 3).wait_send()
        return carry

    lax.fori_loop(0, n_dev, drain, 0)
    for w in (0, 1):
        for t in (1, 2, 3):
            x_copy(w, t).wait_send()


def cache_kernel(
    kp_hbm, vp_hbm, y_hbm, wk_ref, wv_ref, bv_ref, k_hbm, v_hbm,
    wt, bias, y_s, kept_s, new_s, y_sem, kept_sem, new_sem,
):
    layers, _, cols = wk_ref.shape
    chips, frames, _ = y_s.shape
    pieces = new_sem.shape[1]
    piece = frames // pieces
    y_in = [
        [
            pltpu.make_async_copy(
                y_hbm.at[chips + i, pl.ds(p * piece, piece)], y_s.at[i, pl.ds(p * piece, piece)], y_sem.at[i, p]
            )
            for p in range(pieces)
        ]
        for i in range(chips)
    ]
    moves = [
        [
            (
                pltpu.make_async_copy(src.at[:, i], kept_s.at[i, n], kept_sem.at[0, i, n]),
                pltpu.make_async_copy(kept_s.at[i, n], dst.at[:, i], kept_sem.at[1, i, n]),
            )
            for n, (src, dst) in enumerate(((kp_hbm, k_hbm), (vp_hbm, v_hbm)))
        ]
        for i in range(chips)
    ]

    def new(i, p, n):
        at = pl.ds(p * piece, piece)
        dst = (k_hbm, v_hbm)[n]
        return pltpu.make_async_copy(new_s.at[i, n, :, :, at], dst.at[:, chips + i, :, at], new_sem.at[i, p, n])

    y_in, moves = sum(y_in, []), sum(moves, [])
    ahead, lag = 3, 2
    for c in y_in[:ahead]:
        c.start()
    cache_weights(wk_ref, wv_ref, bv_ref, wt, bias)
    for t in range(chips * pieces):
        i, p = t // pieces, t % pieces
        at = slice(p * piece, (p + 1) * piece)
        y_in[t].wait()
        if t + ahead < len(y_in):
            y_in[t + ahead].start()
        for m in range(t * len(moves) // len(y_in), (t + 1) * len(moves) // len(y_in)):
            moves[m][0].start()
        for n, x in enumerate(cache_rows(y_s[i, at], wt, bias)):
            for l in range(layers):
                new_s[i, n, l, :, at] = x[l * cols : (l + 1) * cols]
            new(i, p, n).start()
        if t >= lag:
            for m in range((t - lag) * len(moves) // len(y_in), (t - lag + 1) * len(moves) // len(y_in)):
                moves[m][0].wait()
                moves[m][1].start()
    for m in range((len(y_in) - lag) * len(moves) // len(y_in), len(moves)):
        moves[m][0].wait()
        moves[m][1].start()
    for _, store in moves:
        store.wait()
    for i in range(chips):
        for p in range(pieces):
            for n in (0, 1):
                new(i, p, n).wait()


def solution(mesh):
    n_dev = mesh.shape["sp"]

    def device_fn(x, ln1_gain, ln1_bias, w_query, b_query, w_key, w_value, b_value, w_out, b_out, ln2_gain, ln2_bias, w_up, b_up, w_down, b_down, lnp_gain, lnp_bias, cross_wk, cross_wv, cross_bv):
        clips, rows, d_model = x.shape
        d_ff = w_up.shape[1]
        frames = rows * n_dev
        layers, _, cols = cross_wk.shape
        pairs = d_model // 128
        row = lambda a: a
        hbm = pl.BlockSpec(memory_space=pl.ANY)
        vmem = pl.BlockSpec(memory_space=pltpu.VMEM)
        dma = pltpu.SemaphoreType.DMA
        shape = (layers, clips, cols, frames)
        chips = n_dev // 2
        chunk = 2 * rows
        y_all, k_part, v_part = pl.pallas_call(
            functools.partial(encoder_kernel, n_dev=n_dev, rows=rows),
            out_shape=[jax.ShapeDtypeStruct((clips, frames, d_model), BF16)] + [jax.ShapeDtypeStruct(shape, BF16)] * 2,
            in_specs=[hbm] * 9 + [vmem] * 12,
            out_specs=[hbm] * 3,
            scratch_shapes=[
                pltpu.VMEM((2, n_dev // 2, rows, d_model), BF16),
                pltpu.VMEM((d_model, d_model), BF16),
                pltpu.VMEM((d_model, d_model), BF16),
                pltpu.VMEM((d_model, d_model), BF16),
                pltpu.VMEM((d_model, d_model), BF16),
                pltpu.VMEM((d_model, d_ff), BF16),
                pltpu.VMEM((d_ff, d_model), BF16),
                pltpu.VMEM((2 * pairs, 128, frames // 2), BF16),
                pltpu.VMEM((pairs, frames, 128), BF16),
                pltpu.VMEM((2 * pairs, V_ROWS, frames), BF16),
                pltpu.VMEM((2, frames, rows), F32),
                pltpu.VMEM((2, frames, rows), F32),
                pltpu.VMEM((2, 2, 8, rows), F32),
                pltpu.VMEM((d_model, rows), BF16),
                pltpu.VMEM((2, rows, d_model), BF16),
                pltpu.VMEM((layers, d_model, cols), BF16),
                pltpu.VMEM((layers, d_model, cols), BF16),
                pltpu.VMEM((2 * layers * cols, d_model), BF16),
                pltpu.VMEM((layers * cols, cols), F32),
                pltpu.VMEM((4, chunk, d_model), BF16),
                pltpu.VMEM((2, 2, layers, cols, chunk), BF16),
                dma((2, n_dev // 2)),
                dma((2, n_dev // 2)),
                dma((2, n_dev // 2)),
                dma((2, n_dev // 2)),
                pltpu.SemaphoreType.REGULAR,
                dma((3, 2)),
                dma((4, n_dev)),
                dma((n_dev, n_dev)),
                dma((10,)),
                dma((2,)),
                dma((4,)),
                dma((2, 2)),
            ],
            compiler_params=pltpu.CompilerParams(
                collective_id=0, has_side_effects=True, vmem_limit_bytes=67043328
            ),
            name="encoder",
        )(
            x, w_query, w_key, w_value, w_out, w_up, w_down, cross_wk, cross_wv,
            row(ln1_gain), row(ln1_bias), row(b_query), row(b_value), row(b_out), row(ln2_gain), row(ln2_bias),
            row(b_up), row(b_down), row(lnp_gain), row(lnp_bias), cross_bv,
        )
        pieces = 2
        k, v = pl.pallas_call(
            cache_kernel,
            out_shape=[jax.ShapeDtypeStruct(shape, BF16)] * 2,
            in_specs=[hbm] * 3 + [vmem] * 3,
            out_specs=[hbm] * 2,
            scratch_shapes=[
                pltpu.VMEM((2 * layers * cols, d_model), BF16),
                pltpu.VMEM((layers * cols, cols), F32),
                pltpu.VMEM((chips, frames, d_model), BF16),
                pltpu.VMEM((chips, 2, layers, cols, frames), BF16),
                pltpu.VMEM((chips, 2, layers, cols, frames), BF16),
                dma((chips, pieces)),
                dma((2, chips, 2)),
                dma((chips, pieces, 2)),
            ],
            compiler_params=pltpu.CompilerParams(vmem_limit_bytes=67043328),
            name="caches",
        )(k_part, v_part, y_all, cross_wk, cross_wv, cross_bv)
        heads = lambda a: a.reshape(layers, clips, cols // HEAD_DIM, HEAD_DIM, frames).transpose(0, 1, 4, 2, 3)
        return heads(k), heads(v)

    in_specs = (P("dp", "sp", None),) + (P(),) * 17 + (P(None, None, "sp"), P(None, None, "sp"), P(None, "sp"))
    out_specs = (P(None, "dp", None, "sp", None), P(None, "dp", None, "sp", None))
    return jax.shard_map(device_fn, mesh=mesh, in_specs=in_specs, out_specs=out_specs, check_vma=False)
```

```python
import functools
import math

import jax
import jax.numpy as jnp
from jax import lax
from jax.experimental import pallas as pl
from jax.experimental.pallas import tpu as pltpu
from jax.sharding import PartitionSpec as P

HEAD_DIM = 64
LN_EPS = 1e-5
LOG2E = math.log2(math.e)
V_ROWS = 80
F32 = jnp.float32
BF16 = jnp.bfloat16


def layer_norm(h, gain, bias):
    mean = jnp.mean(h, axis=-1, keepdims=True)
    centered = h - mean
    var = jnp.mean(centered * centered, axis=-1, keepdims=True)
    return centered * lax.rsqrt(var + LN_EPS) * gain + bias


def wide(row):
    return row.astype(F32).reshape(1, -1)


def dot(a, b, ca=1, cb=0):
    return lax.dot_general(a, b, (((ca,), (cb,)), ((), ())), preferred_element_type=F32)


def cache_weights(wk_ref, wv_ref, bv_ref, wt, bias):
    layers, _, cols = wk_ref.shape
    for i in range(layers):
        wt[i * cols : (i + 1) * cols, :] = wk_ref[i].T
        wt[(layers + i) * cols : (layers + i + 1) * cols, :] = wv_ref[i].T
        bias[i * cols : (i + 1) * cols, :] = jnp.broadcast_to(bv_ref[i : i + 1, :].astype(F32), (cols, cols)).T


def cache_rows(y, wt, bias):
    half = bias.shape[0]
    out = dot(wt[...], y, 1, 1)
    return out[:half].astype(BF16), (out[half:] + bias[:, :1]).astype(BF16)


def encoder_kernel(
    x_hbm, wq_hbm, wk_hbm, wv_hbm, wo_hbm, w1_hbm, w2_hbm, ck_hbm, cv_hbm,
    g1_ref, c1_ref, bq_ref, bv_ref, bo_ref, g2_ref, c2_ref, b1_ref, b2_ref, gp_ref, cp_ref, cb_ref,
    y_hbm, kp_hbm, vp_hbm,
    xc, wq, wk, wv, wo, w1, w2, q_s, k_s, v_s, sa, sb, mx_s, o_s, y_s, ck_s, cv_s, wt_s, bias_s, cy_s, co_s,
    x_send, x_recv, kv_send, kv_recv, credit, y_send, f_send, y_recv, load_sem, y_loc, c_load, c_store,
    *, n_dev, rows,
):
    d_model = wq.shape[0]
    d_ff = w1.shape[1]
    pairs = d_model // 128
    frames = n_dev * rows
    scale = HEAD_DIM**-0.25
    me = lax.axis_index("sp")
    core = me % 2
    px = (me // 2) % 2
    py = me // 4

    def flip(t):
        c = core + (t % 2) * (1 - 2 * core)
        x = px + ((t // 2) % 2) * (1 - 2 * px)
        y = py + (t // 4) * (1 - 2 * py)
        return y * 4 + x * 2 + c

    near, across_x, across_y, diag = flip(1), flip(2), flip(4), flip(6)

    barrier = pltpu.get_barrier_semaphore()
    for dev in (near, across_x, across_y, diag):
        pl.semaphore_signal(barrier, inc=1, device_id={"sp": dev}, device_id_type=pl.DeviceIdType.MESH)
    pl.semaphore_wait(barrier, 4)

    chips = n_dev // 2
    chip = me // 2

    def x_copy(w, t):
        dev = flip(2 * t)
        return pltpu.make_async_remote_copy(
            src_ref=x_hbm.at[w * chips + dev // 2], dst_ref=xc.at[w, chip],
            send_sem=x_send.at[w, t], recv_sem=x_recv.at[w, chip],
            device_id={"sp": dev}, device_id_type=pl.DeviceIdType.MESH,
        )

    def x_arrival(w, slot):
        return pltpu.make_async_remote_copy(
            src_ref=x_hbm.at[0], dst_ref=xc.at[w, slot], send_sem=x_send.at[w, 0], recv_sem=x_recv.at[w, slot],
            device_id={"sp": near}, device_id_type=pl.DeviceIdType.MESH,
        )

    own_x = [pltpu.make_async_copy(x_hbm.at[w * chips + chip], xc.at[w, chip], load_sem.at[8 + w]) for w in (0, 1)]
    own_x[0].start()
    for t in (1, 2, 3):
        x_copy(0, t).start()
    loads = [
        pltpu.make_async_copy(a, b, load_sem.at[i])
        for i, (a, b) in enumerate(
            ((wq_hbm, wq), (wk_hbm, wk), (wv_hbm, wv), (wo_hbm, wo), (w1_hbm, w1), (w2_hbm, w2), (ck_hbm, ck_s), (cv_hbm, cv_s))
        )
    ]
    for c in loads:
        c.start()
    own_x[1].start()

    ones = (lax.broadcasted_iota(jnp.int32, (V_ROWS - HEAD_DIM, frames), 0) == 0).astype(BF16)
    q_zero = jnp.zeros((HEAD_DIM, chips * rows), BF16)
    for h in range(2 * pairs):
        v_s[h, HEAD_DIM:, :] = ones
        q_s[h, HEAD_DIM * (1 - h % 2) : HEAD_DIM * (2 - h % 2), :] = q_zero

    for c in (*own_x, *loads[:3], *loads[6:]):
        c.wait()
    cache_weights(ck_s, cv_s, cb_ref, wt_s, bias_s)

    def kv_copies(s):
        at = pl.ds(pl.multiple_of((core * chips + s) * rows, rows), rows)
        return [
            pltpu.make_async_remote_copy(
                src_ref=ref, dst_ref=ref, send_sem=kv_send.at[i, s], recv_sem=kv_recv.at[i, s],
                device_id={"sp": near}, device_id_type=pl.DeviceIdType.MESH,
            )
            for i, ref in enumerate((k_s.at[:, at, :], v_s.at[:, pl.ds(0, HEAD_DIM), at]))
        ]

    def project(w, t):
        slot = flip(2 * t) // 2

        @pl.when((w == 0) & (t == chips - 1))
        def _():
            for i in (1, 2, 3):
                x_copy(1, i).start()

        @pl.when(t > 0)
        def _():
            x_arrival(w, slot).wait_recv()

        a = layer_norm(xc[w, slot].astype(F32), wide(g1_ref[...]), wide(c1_ref[...])).astype(BF16)
        at_q = pl.multiple_of(slot * rows, rows)
        at = pl.multiple_of((core * chips + slot) * rows, rows)
        q = ((dot(a, wq[...]) + wide(bq_ref[...])) * scale).astype(BF16).T
        k = (dot(a, wk[...]) * scale).astype(BF16)
        for p in range(pairs):
            for half in (0, 1):
                h = 2 * p + half
                own_rows = slice(half * HEAD_DIM, (half + 1) * HEAD_DIM)
                q_s[h, own_rows, pl.ds(at_q, rows)] = q[h * HEAD_DIM : (h + 1) * HEAD_DIM]
            k_s[p, pl.ds(at, rows), :] = k[:, p * 128 : (p + 1) * 128]
        v = (dot(a, wv[...]) + wide(bv_ref[...])).astype(BF16).T
        for h in range(2 * pairs):
            v_s[h, :HEAD_DIM, pl.ds(at, rows)] = v[h * HEAD_DIM : (h + 1) * HEAD_DIM]

        @pl.when((w == 1) & (t == 0))
        def _():
            pl.semaphore_wait(credit, 1)

        for c in kv_copies(slot):
            c.start()

    kc = 256

    def y_block(src, j):
        clip = (j // chips) * chips + src // 2
        return y_hbm.at[clip, pl.ds(pl.multiple_of((2 * (j % chips) + src % 2) * rows, rows), rows)]

    def y_copy(src_ref, src, j, dst_dev, sem):
        return pltpu.make_async_remote_copy(
            src_ref=src_ref, dst_ref=y_block(src, j),
            send_sem=sem, recv_sem=y_recv.at[src, j],
            device_id={"sp": dst_dev}, device_id_type=pl.DeviceIdType.MESH,
        )

    def forward(src, j, dst_dev, kind):
        return y_copy(y_block(src, j), src, j, dst_dev, f_send.at[kind, j])

    def arrived(src, j):
        y_copy(y_block(src, j), src, j, near, f_send.at[0, j]).wait_recv()

    def own(j, kind, dst_dev):
        return y_copy(y_s.at[j % 2], me, j, dst_dev, y_send.at[kind, j % 2])

    def store_own(j):
        return pltpu.make_async_copy(y_s.at[j % 2], y_block(me, j), y_loc.at[j % 2])

    def relay_first(j):
        arrived(across_x, j)
        arrived(across_y, j)
        forward(across_x, j, near, 0).start()
        forward(across_y, j, near, 1).start()
        via, to = (1 - core) * across_x + core * across_y, (1 - core) * across_y + core * across_x
        forward(via, j, to, 2).start()

    def relay_second(j):
        arrived(diag, j)
        forward(diag, j, near, 3).start()

    def score_chunk(pair, q, s_ref, half, c, mx):
        at = slice(c * kc, (c + 1) * kc)
        x = dot(k_s[pair, at, :], q)
        s_ref[half, at, :] = x
        return jnp.maximum(mx, jnp.max(x.reshape(kc // 8, 8, rows), axis=0))

    def queries(pair, s):
        at = pl.ds(pl.multiple_of(s * rows, rows), rows)
        return [q_s[2 * pair + half, :, at] for half in (0, 1)]

    mx0 = jnp.full((8, rows), -jnp.inf, F32)

    def first_scores():
        q = queries(0, 0)
        for half in (0, 1):
            mx = mx0
            for c in range(frames // kc):
                mx = score_chunk(0, q[half], sa, half, c, mx)
            mx_s[0, half] = mx

    def attend(pair, cur, cur_mx, next_pair, next_s, nxt, nxt_mx):
        top = [jnp.max(mx_s[cur_mx, half], axis=0, keepdims=True) * LOG2E for half in (0, 1)]
        q = queries(next_pair, next_s)
        mx = [mx0, mx0]
        o = [jnp.zeros((V_ROWS, rows), F32)] * 2
        for c in range(frames // kc):
            at = slice(c * kc, (c + 1) * kc)
            for half in (0, 1):
                mx[half] = score_chunk(next_pair, q[half], nxt, half, c, mx[half])
                p = jnp.exp2(cur[half, at, :] * LOG2E - top[half]).astype(BF16)
                o[half] = o[half] + dot(v_s[2 * pair + half, :, at], p)
        for half in (0, 1):
            mx_s[nxt_mx, half] = mx[half]
            out = (o[half][:HEAD_DIM] * (1.0 / o[half][HEAD_DIM : HEAD_DIM + 1])).astype(BF16)
            o_s[pl.ds(pl.multiple_of(pair * 128 + half * HEAD_DIM, HEAD_DIM), HEAD_DIM), :] = out

    def step(w, s):
        j = w * chips + s

        def two_pairs(i, carry):
            pair = 2 * i
            wrap = (pair + 2) // pairs

            @pl.when(i >= 0)
            def _():
                attend(pair, sa, 0, pair + 1, s, sb, 1)

            @pl.when(i < pairs)
            def _():
                attend(pair + 1, sb, 1, (pair + 2) % pairs, jnp.minimum(s + wrap, chips - 1), sa, 0)

            return carry

        lax.fori_loop(0, pairs // 2, two_pairs, 0)

        @pl.when(j == chips)
        def _():
            relay_first(j - 1)

        h = xc[w, s].astype(F32) + dot(o_s[...].T, wo[...]) + wide(bo_ref[...])
        n = layer_norm(h, wide(g2_ref[...]), wide(c2_ref[...])).astype(BF16)
        h = h + wide(b2_ref[...])
        fc = 1024
        for c in range(d_ff // fc):
            u = dot(n, w1[:, c * fc : (c + 1) * fc]) + wide(b1_ref[c * fc : (c + 1) * fc])
            u = (0.5 * u * (1.0 + lax.erf(u * math.sqrt(0.5)))).astype(BF16)
            h = h + dot(u, w2[c * fc : (c + 1) * fc, :])
        y = layer_norm(h, wide(gp_ref[...]), wide(cp_ref[...])).astype(BF16)

        @pl.when(j >= 2)
        def _():
            for kind, dev in enumerate((near, across_x, across_y)):
                own(j - 2, kind, dev).wait_send()
            store_own(j - 2).wait()

        y_s[j % 2] = y
        for kind, dev in ((1, across_x), (2, across_y), (0, near)):
            own(j, kind, dev).start()
        store_own(j).start()

        @pl.when((j >= 1) & (j != chips - 1) & (j != chips))
        def _():
            relay_first(j - 1)

        @pl.when(j >= 3)
        def _():
            relay_second(j - 3)

    def wave(w, carry):
        lax.fori_loop(0, chips, lambda t, c: (project(w, t), c)[1], 0)

        @pl.when(w == 0)
        def _():
            for c in loads[3:6]:
                c.wait()

        @pl.when(w == 1)
        def _():
            relay_first(chips - 2)

        for s in range(chips):
            for c in kv_copies(s):
                c.wait()
        first_scores()
        lax.fori_loop(0, chips, lambda s, c: (step(w, s), c)[1], 0)

        @pl.when(w == 0)
        def _():
            pl.semaphore_signal(credit, inc=1, device_id={"sp": near}, device_id_type=pl.DeviceIdType.MESH)

        return carry

    lax.fori_loop(0, 2, wave, 0)

    last = n_dev - 1
    ahead, chunk = cy_s.shape[:2]
    layers, _, cols = ck_s.shape

    def caches(count, where):
        def load(t):
            clip, at = where(t)
            at = pl.multiple_of(at * chunk, chunk)
            return pltpu.make_async_copy(y_hbm.at[clip, pl.ds(at, chunk)], cy_s.at[t % ahead], c_load.at[t % ahead])

        def stores(t):
            clip, at = where(t)
            at = pl.multiple_of(at * chunk, chunk)
            return [
                pltpu.make_async_copy(co_s.at[t % 2, i], dst.at[:, clip, :, pl.ds(at, chunk)], c_store.at[t % 2, i])
                for i, dst in enumerate((kp_hbm, vp_hbm))
            ]

        for t in range(ahead - 1):
            load(t).start()

        def task(t, carry):
            @pl.when(t + ahead - 1 < count)
            def _():
                load(t + ahead - 1).start()

            @pl.when(t >= 2)
            def _():
                for c in stores(t - 2):
                    c.wait()

            load(t).wait()
            for i, x in enumerate(cache_rows(cy_s[t % ahead], wt_s, bias_s)):
                for l in range(layers):
                    co_s[t % 2, i, l] = x[l * cols : (l + 1) * cols]
            for c in stores(t):
                c.start()
            return carry

        lax.fori_loop(0, count, task, 0)
        for t in (count - 2, count - 1):
            for c in stores(t):
                c.wait()

    def near_arrived(first, end):
        def wait(j, carry):
            for t in (1, 3, 5, 7):
                arrived(flip(t), j)
            return carry

        lax.fori_loop(first, end, wait, 0)

    def own_done(j):
        for kind, dev in enumerate((near, across_x, across_y)):
            own(j, kind, dev).wait_send()
        store_own(j).wait()

    relay_second(last - 2)
    near_arrived(0, chips)
    caches(10, lambda t: (t // chips, t % chips))
    relay_first(last)
    caches(6, lambda t: ((t + 10) // chips, (t + 10) % chips))

    relay_second(last - 1)
    relay_second(last)
    own_done(last - 1)
    own_done(last)
    near_arrived(chips, n_dev)

    def drain(j, carry):
        forward(across_x, j, near, 0).wait_send()
        forward(across_y, j, near, 1).wait_send()
        forward(across_x, j, across_y, 2).wait_send()
        forward(diag, j, near, 3).wait_send()
        return carry

    lax.fori_loop(0, n_dev, drain, 0)
    for w in (0, 1):
        for t in (1, 2, 3):
            x_copy(w, t).wait_send()


def cache_kernel(
    kp_hbm, vp_hbm, y_hbm, wk_ref, wv_ref, bv_ref, k_hbm, v_hbm,
    wt, bias, y_s, kept_s, new_s, y_sem, kept_sem, new_sem,
):
    layers, _, cols = wk_ref.shape
    chips, frames, _ = y_s.shape
    pieces = new_sem.shape[1]
    piece = frames // pieces
    y_in = [
        [
            pltpu.make_async_copy(
                y_hbm.at[chips + i, pl.ds(p * piece, piece)], y_s.at[i, pl.ds(p * piece, piece)], y_sem.at[i, p]
            )
            for p in range(pieces)
        ]
        for i in range(chips)
    ]
    moves = [
        [
            (
                pltpu.make_async_copy(src.at[:, i], kept_s.at[i, n], kept_sem.at[0, i, n]),
                pltpu.make_async_copy(kept_s.at[i, n], dst.at[:, i], kept_sem.at[1, i, n]),
            )
            for n, (src, dst) in enumerate(((kp_hbm, k_hbm), (vp_hbm, v_hbm)))
        ]
        for i in range(chips)
    ]

    def new(i, p, n):
        at = pl.ds(p * piece, piece)
        dst = (k_hbm, v_hbm)[n]
        return pltpu.make_async_copy(new_s.at[i, n, :, :, at], dst.at[:, chips + i, :, at], new_sem.at[i, p, n])

    y_in, moves = sum(y_in, []), sum(moves, [])
    ahead, lag = 3, 2
    for c in y_in[:ahead]:
        c.start()
    cache_weights(wk_ref, wv_ref, bv_ref, wt, bias)
    for t in range(chips * pieces):
        i, p = t // pieces, t % pieces
        at = slice(p * piece, (p + 1) * piece)
        y_in[t].wait()
        if t + ahead < len(y_in):
            y_in[t + ahead].start()
        for m in range(t * len(moves) // len(y_in), (t + 1) * len(moves) // len(y_in)):
            moves[m][0].start()
        for n, x in enumerate(cache_rows(y_s[i, at], wt, bias)):
            for l in range(layers):
                new_s[i, n, l, :, at] = x[l * cols : (l + 1) * cols]
            new(i, p, n).start()
        if t >= lag:
            for m in range((t - lag) * len(moves) // len(y_in), (t - lag + 1) * len(moves) // len(y_in)):
                moves[m][0].wait()
                moves[m][1].start()
    for m in range((len(y_in) - lag) * len(moves) // len(y_in), len(moves)):
        moves[m][0].wait()
        moves[m][1].start()
    for _, store in moves:
        store.wait()
    for i in range(chips):
        for p in range(pieces):
            for n in (0, 1):
                new(i, p, n).wait()


def solution(mesh):
    n_dev = mesh.shape["sp"]

    def device_fn(x, ln1_gain, ln1_bias, w_query, b_query, w_key, w_value, b_value, w_out, b_out, ln2_gain, ln2_bias, w_up, b_up, w_down, b_down, lnp_gain, lnp_bias, cross_wk, cross_wv, cross_bv):
        clips, rows, d_model = x.shape
        d_ff = w_up.shape[1]
        frames = rows * n_dev
        layers, _, cols = cross_wk.shape
        pairs = d_model // 128
        row = lambda a: a
        hbm = pl.BlockSpec(memory_space=pl.ANY)
        vmem = pl.BlockSpec(memory_space=pltpu.VMEM)
        dma = pltpu.SemaphoreType.DMA
        shape = (layers, clips, cols, frames)
        chips = n_dev // 2
        chunk = 2 * rows
        y_all, k_part, v_part = pl.pallas_call(
            functools.partial(encoder_kernel, n_dev=n_dev, rows=rows),
            out_shape=[jax.ShapeDtypeStruct((clips, frames, d_model), BF16)] + [jax.ShapeDtypeStruct(shape, BF16)] * 2,
            in_specs=[hbm] * 9 + [vmem] * 12,
            out_specs=[hbm] * 3,
            scratch_shapes=[
                pltpu.VMEM((2, n_dev // 2, rows, d_model), BF16),
                pltpu.VMEM((d_model, d_model), BF16),
                pltpu.VMEM((d_model, d_model), BF16),
                pltpu.VMEM((d_model, d_model), BF16),
                pltpu.VMEM((d_model, d_model), BF16),
                pltpu.VMEM((d_model, d_ff), BF16),
                pltpu.VMEM((d_ff, d_model), BF16),
                pltpu.VMEM((2 * pairs, 128, frames // 2), BF16),
                pltpu.VMEM((pairs, frames, 128), BF16),
                pltpu.VMEM((2 * pairs, V_ROWS, frames), BF16),
                pltpu.VMEM((2, frames, rows), F32),
                pltpu.VMEM((2, frames, rows), F32),
                pltpu.VMEM((2, 2, 8, rows), F32),
                pltpu.VMEM((d_model, rows), BF16),
                pltpu.VMEM((2, rows, d_model), BF16),
                pltpu.VMEM((layers, d_model, cols), BF16),
                pltpu.VMEM((layers, d_model, cols), BF16),
                pltpu.VMEM((2 * layers * cols, d_model), BF16),
                pltpu.VMEM((layers * cols, cols), F32),
                pltpu.VMEM((4, chunk, d_model), BF16),
                pltpu.VMEM((2, 2, layers, cols, chunk), BF16),
                dma((2, n_dev // 2)),
                dma((2, n_dev // 2)),
                dma((2, n_dev // 2)),
                dma((2, n_dev // 2)),
                pltpu.SemaphoreType.REGULAR,
                dma((3, 2)),
                dma((4, n_dev)),
                dma((n_dev, n_dev)),
                dma((10,)),
                dma((2,)),
                dma((4,)),
                dma((2, 2)),
            ],
            compiler_params=pltpu.CompilerParams(
                collective_id=0, has_side_effects=True, vmem_limit_bytes=67043328
            ),
            name="encoder",
        )(
            x, w_query, w_key, w_value, w_out, w_up, w_down, cross_wk, cross_wv,
            row(ln1_gain), row(ln1_bias), row(b_query), row(b_value), row(b_out), row(ln2_gain), row(ln2_bias),
            row(b_up), row(b_down), row(lnp_gain), row(lnp_bias), cross_bv,
        )
        pieces = 2
        k, v = pl.pallas_call(
            cache_kernel,
            out_shape=[jax.ShapeDtypeStruct(shape, BF16)] * 2,
            in_specs=[hbm] * 3 + [vmem] * 3,
            out_specs=[hbm] * 2,
            scratch_shapes=[
                pltpu.VMEM((2 * layers * cols, d_model), BF16),
                pltpu.VMEM((layers * cols, cols), F32),
                pltpu.VMEM((chips, frames, d_model), BF16),
                pltpu.VMEM((chips, 2, layers, cols, frames), BF16),
                pltpu.VMEM((chips, 2, layers, cols, frames), BF16),
                dma((chips, pieces)),
                dma((2, chips, 2)),
                dma((chips, pieces, 2)),
            ],
            compiler_params=pltpu.CompilerParams(vmem_limit_bytes=67043328),
            name="caches",
        )(k_part, v_part, y_all, cross_wk, cross_wv, cross_bv)
        heads = lambda a: a.reshape(layers, clips, cols // HEAD_DIM, HEAD_DIM, frames).transpose(0, 1, 4, 2, 3)
        return heads(k), heads(v)

    in_specs = (P("dp", "sp", None),) + (P(),) * 17 + (P(None, None, "sp"), P(None, None, "sp"), P(None, "sp"))
    out_specs = (P(None, "dp", None, "sp", None), P(None, "dp", None, "sp", None))
    return jax.shard_map(device_fn, mesh=mesh, in_specs=in_specs, out_specs=out_specs, check_vma=False)
```

```python
import functools
import math

import jax
import jax.numpy as jnp
from jax import lax
from jax.experimental import pallas as pl
from jax.experimental.pallas import tpu as pltpu
from jax.sharding import PartitionSpec as P

HEAD_DIM = 64
LN_EPS = 1e-5
LOG2E = math.log2(math.e)
V_ROWS = 80
F32 = jnp.float32
BF16 = jnp.bfloat16


def layer_norm(h, gain, bias):
    mean = jnp.mean(h, axis=-1, keepdims=True)
    centered = h - mean
    var = jnp.mean(centered * centered, axis=-1, keepdims=True)
    return centered * lax.rsqrt(var + LN_EPS) * gain + bias


def wide(row):
    return row.astype(F32).reshape(1, -1)


def dot(a, b, ca=1, cb=0):
    return lax.dot_general(a, b, (((ca,), (cb,)), ((), ())), preferred_element_type=F32)


def cache_weights(wk_ref, wv_ref, bv_ref, wt, bias):
    layers, _, cols = wk_ref.shape
    for i in range(layers):
        wt[i * cols : (i + 1) * cols, :] = wk_ref[i].T
        wt[(layers + i) * cols : (layers + i + 1) * cols, :] = wv_ref[i].T
        bias[i * cols : (i + 1) * cols, :] = jnp.broadcast_to(bv_ref[i : i + 1, :].astype(F32), (cols, cols)).T


def cache_rows(y, wt, bias):
    half = bias.shape[0]
    out = dot(wt[...], y, 1, 1)
    return out[:half].astype(BF16), (out[half:] + bias[:, :1]).astype(BF16)


def encoder_kernel(
    x_hbm, wq_hbm, wk_hbm, wv_hbm, wo_hbm, w1_hbm, w2_hbm, ck_hbm, cv_hbm,
    g1_ref, c1_ref, bq_ref, bv_ref, bo_ref, g2_ref, c2_ref, b1_ref, b2_ref, gp_ref, cp_ref, cb_ref,
    y_hbm, kp_hbm, vp_hbm,
    xc, wq, wk, wv, wo, w1, w2, q_s, k_s, v_s, sa, sb, mx_s, o_s, y_s, ck_s, cv_s, wt_s, bias_s, cy_s, co_s,
    x_send, x_recv, kv_send, kv_recv, credit, y_send, f_send, y_recv, load_sem, y_loc, c_load, c_store,
    *, n_dev, rows,
):
    d_model = wq.shape[0]
    d_ff = w1.shape[1]
    pairs = d_model // 128
    frames = n_dev * rows
    scale = HEAD_DIM**-0.25
    me = lax.axis_index("sp")
    core = me % 2
    px = (me // 2) % 2
    py = me // 4

    def flip(t):
        c = core + (t % 2) * (1 - 2 * core)
        x = px + ((t // 2) % 2) * (1 - 2 * px)
        y = py + (t // 4) * (1 - 2 * py)
        return y * 4 + x * 2 + c

    near, across_x, across_y, diag = flip(1), flip(2), flip(4), flip(6)

    barrier = pltpu.get_barrier_semaphore()
    for dev in (near, across_x, across_y, diag):
        pl.semaphore_signal(barrier, inc=1, device_id={"sp": dev}, device_id_type=pl.DeviceIdType.MESH)
    pl.semaphore_wait(barrier, 4)

    chips = n_dev // 2
    chip = me // 2

    def x_copy(w, t):
        dev = flip(2 * t)
        return pltpu.make_async_remote_copy(
            src_ref=x_hbm.at[w * chips + dev // 2], dst_ref=xc.at[w, chip],
            send_sem=x_send.at[w, t], recv_sem=x_recv.at[w, chip],
            device_id={"sp": dev}, device_id_type=pl.DeviceIdType.MESH,
        )

    def x_arrival(w, slot):
        return pltpu.make_async_remote_copy(
            src_ref=x_hbm.at[0], dst_ref=xc.at[w, slot], send_sem=x_send.at[w, 0], recv_sem=x_recv.at[w, slot],
            device_id={"sp": near}, device_id_type=pl.DeviceIdType.MESH,
        )

    own_x = [pltpu.make_async_copy(x_hbm.at[w * chips + chip], xc.at[w, chip], load_sem.at[8 + w]) for w in (0, 1)]
    own_x[0].start()
    for t in (1, 2, 3):
        x_copy(0, t).start()
    loads = [
        pltpu.make_async_copy(a, b, load_sem.at[i])
        for i, (a, b) in enumerate(
            ((wq_hbm, wq), (wk_hbm, wk), (wv_hbm, wv), (wo_hbm, wo), (w1_hbm, w1), (w2_hbm, w2), (ck_hbm, ck_s), (cv_hbm, cv_s))
        )
    ]
    for c in loads:
        c.start()
    own_x[1].start()

    ones = (lax.broadcasted_iota(jnp.int32, (V_ROWS - HEAD_DIM, frames), 0) == 0).astype(BF16)
    q_zero = jnp.zeros((HEAD_DIM, chips * rows), BF16)
    for h in range(2 * pairs):
        v_s[h, HEAD_DIM:, :] = ones
        q_s[h, HEAD_DIM * (1 - h % 2) : HEAD_DIM * (2 - h % 2), :] = q_zero

    for c in (*own_x, *loads[:3], *loads[6:]):
        c.wait()
    cache_weights(ck_s, cv_s, cb_ref, wt_s, bias_s)

    def kv_copies(s):
        at = pl.ds(pl.multiple_of((core * chips + s) * rows, rows), rows)
        return [
            pltpu.make_async_remote_copy(
                src_ref=ref, dst_ref=ref, send_sem=kv_send.at[i, s], recv_sem=kv_recv.at[i, s],
                device_id={"sp": near}, device_id_type=pl.DeviceIdType.MESH,
            )
            for i, ref in enumerate((k_s.at[:, at, :], v_s.at[:, pl.ds(0, HEAD_DIM), at]))
        ]

    def project(w, t):
        slot = flip(2 * t) // 2

        @pl.when((w == 0) & (t == chips - 1))
        def _():
            for i in (1, 2, 3):
                x_copy(1, i).start()

        @pl.when(t > 0)
        def _():
            x_arrival(w, slot).wait_recv()

        a = layer_norm(xc[w, slot].astype(F32), wide(g1_ref[...]), wide(c1_ref[...])).astype(BF16)
        at_q = pl.multiple_of(slot * rows, rows)
        at = pl.multiple_of((core * chips + slot) * rows, rows)
        q = ((dot(a, wq[...]) + wide(bq_ref[...])) * scale).astype(BF16).T
        k = (dot(a, wk[...]) * scale).astype(BF16)
        for p in range(pairs):
            for half in (0, 1):
                h = 2 * p + half
                own_rows = slice(half * HEAD_DIM, (half + 1) * HEAD_DIM)
                q_s[h, own_rows, pl.ds(at_q, rows)] = q[h * HEAD_DIM : (h + 1) * HEAD_DIM]
            k_s[p, pl.ds(at, rows), :] = k[:, p * 128 : (p + 1) * 128]
        v = (dot(a, wv[...]) + wide(bv_ref[...])).astype(BF16).T
        for h in range(2 * pairs):
            v_s[h, :HEAD_DIM, pl.ds(at, rows)] = v[h * HEAD_DIM : (h + 1) * HEAD_DIM]

        @pl.when((w == 1) & (t == 0))
        def _():
            pl.semaphore_wait(credit, 1)

        for c in kv_copies(slot):
            c.start()

    kc = 256

    def y_block(src, j):
        clip = (j // chips) * chips + src // 2
        return y_hbm.at[clip, pl.ds(pl.multiple_of((2 * (j % chips) + src % 2) * rows, rows), rows)]

    def y_copy(src_ref, src, j, dst_dev, sem):
        return pltpu.make_async_remote_copy(
            src_ref=src_ref, dst_ref=y_block(src, j),
            send_sem=sem, recv_sem=y_recv.at[src, j],
            device_id={"sp": dst_dev}, device_id_type=pl.DeviceIdType.MESH,
        )

    def forward(src, j, dst_dev, kind):
        return y_copy(y_block(src, j), src, j, dst_dev, f_send.at[kind, j])

    def arrived(src, j):
        y_copy(y_block(src, j), src, j, near, f_send.at[0, j]).wait_recv()

    def own(j, kind, dst_dev):
        return y_copy(y_s.at[j % 2], me, j, dst_dev, y_send.at[kind, j % 2])

    def store_own(j):
        return pltpu.make_async_copy(y_s.at[j % 2], y_block(me, j), y_loc.at[j % 2])

    def relay_first(j):
        arrived(across_x, j)
        arrived(across_y, j)
        forward(across_x, j, near, 0).start()
        forward(across_y, j, near, 1).start()
        via, to = (1 - core) * across_x + core * across_y, (1 - core) * across_y + core * across_x
        forward(via, j, to, 2).start()

    def relay_second(j):
        arrived(diag, j)
        forward(diag, j, near, 3).start()

    def score_chunk(pair, q, s_ref, half, c, mx):
        at = slice(c * kc, (c + 1) * kc)
        x = dot(k_s[pair, at, :], q)
        s_ref[half, at, :] = x
        return jnp.maximum(mx, jnp.max(x.reshape(kc // 8, 8, rows), axis=0))

    def queries(pair, s):
        at = pl.ds(pl.multiple_of(s * rows, rows), rows)
        return [q_s[2 * pair + half, :, at] for half in (0, 1)]

    mx0 = jnp.full((8, rows), -jnp.inf, F32)

    def first_scores():
        q = queries(0, 0)
        for half in (0, 1):
            mx = mx0
            for c in range(frames // kc):
                mx = score_chunk(0, q[half], sa, half, c, mx)
            mx_s[0, half] = mx

    def attend(pair, cur, cur_mx, next_pair, next_s, nxt, nxt_mx):
        top = [jnp.max(mx_s[cur_mx, half], axis=0, keepdims=True) * LOG2E for half in (0, 1)]
        q = queries(next_pair, next_s)
        mx = [mx0, mx0]
        o = [jnp.zeros((V_ROWS, rows), F32)] * 2
        for c in range(frames // kc):
            at = slice(c * kc, (c + 1) * kc)
            for half in (0, 1):
                mx[half] = score_chunk(next_pair, q[half], nxt, half, c, mx[half])
                p = jnp.exp2(cur[half, at, :] * LOG2E - top[half]).astype(BF16)
                o[half] = o[half] + dot(v_s[2 * pair + half, :, at], p)
        for half in (0, 1):
            mx_s[nxt_mx, half] = mx[half]
            out = (o[half][:HEAD_DIM] * (1.0 / o[half][HEAD_DIM : HEAD_DIM + 1])).astype(BF16)
            o_s[pl.ds(pl.multiple_of(pair * 128 + half * HEAD_DIM, HEAD_DIM), HEAD_DIM), :] = out

    def step(w, s):
        j = w * chips + s

        def two_pairs(i, carry):
            pair = 2 * i
            wrap = (pair + 2) // pairs

            @pl.when(i >= 0)
            def _():
                attend(pair, sa, 0, pair + 1, s, sb, 1)

            @pl.when(i < pairs)
            def _():
                attend(pair + 1, sb, 1, (pair + 2) % pairs, jnp.minimum(s + wrap, chips - 1), sa, 0)

            return carry

        lax.fori_loop(0, pairs // 2, two_pairs, 0)

        @pl.when(j == chips)
        def _():
            relay_first(j - 1)

        h = xc[w, s].astype(F32) + dot(o_s[...].T, wo[...]) + wide(bo_ref[...])
        n = layer_norm(h, wide(g2_ref[...]), wide(c2_ref[...])).astype(BF16)
        h = h + wide(b2_ref[...])
        fc = 2048
        for c in range(d_ff // fc):
            u = dot(n, w1[:, c * fc : (c + 1) * fc]) + wide(b1_ref[c * fc : (c + 1) * fc])
            u = (0.5 * u * (1.0 + lax.erf(u * math.sqrt(0.5)))).astype(BF16)
            h = h + dot(u, w2[c * fc : (c + 1) * fc, :])
        y = layer_norm(h, wide(gp_ref[...]), wide(cp_ref[...])).astype(BF16)

        @pl.when(j >= 2)
        def _():
            for kind, dev in enumerate((near, across_x, across_y)):
                own(j - 2, kind, dev).wait_send()
            store_own(j - 2).wait()

        y_s[j % 2] = y
        for kind, dev in ((1, across_x), (2, across_y), (0, near)):
            own(j, kind, dev).start()
        store_own(j).start()

        @pl.when((j >= 1) & (j != chips - 1) & (j != chips))
        def _():
            relay_first(j - 1)

        @pl.when(j >= 3)
        def _():
            relay_second(j - 3)

    def wave(w, carry):
        lax.fori_loop(0, chips, lambda t, c: (project(w, t), c)[1], 0)

        @pl.when(w == 0)
        def _():
            for c in loads[3:6]:
                c.wait()

        @pl.when(w == 1)
        def _():
            relay_first(chips - 2)

        for s in range(chips):
            for c in kv_copies(s):
                c.wait()
        first_scores()
        lax.fori_loop(0, chips, lambda s, c: (step(w, s), c)[1], 0)

        @pl.when(w == 0)
        def _():
            pl.semaphore_signal(credit, inc=1, device_id={"sp": near}, device_id_type=pl.DeviceIdType.MESH)

        return carry

    lax.fori_loop(0, 2, wave, 0)

    last = n_dev - 1
    ahead, chunk = cy_s.shape[:2]
    layers, _, cols = ck_s.shape

    def caches(count, where):
        def load(t):
            clip, at = where(t)
            at = pl.multiple_of(at * chunk, chunk)
            return pltpu.make_async_copy(y_hbm.at[clip, pl.ds(at, chunk)], cy_s.at[t % ahead], c_load.at[t % ahead])

        def stores(t):
            clip, at = where(t)
            at = pl.multiple_of(at * chunk, chunk)
            return [
                pltpu.make_async_copy(co_s.at[t % 2, i], dst.at[:, clip, :, pl.ds(at, chunk)], c_store.at[t % 2, i])
                for i, dst in enumerate((kp_hbm, vp_hbm))
            ]

        for t in range(ahead - 1):
            load(t).start()

        def task(t, carry):
            @pl.when(t + ahead - 1 < count)
            def _():
                load(t + ahead - 1).start()

            @pl.when(t >= 2)
            def _():
                for c in stores(t - 2):
                    c.wait()

            load(t).wait()
            for i, x in enumerate(cache_rows(cy_s[t % ahead], wt_s, bias_s)):
                for l in range(layers):
                    co_s[t % 2, i, l] = x[l * cols : (l + 1) * cols]
            for c in stores(t):
                c.start()
            return carry

        lax.fori_loop(0, count, task, 0)
        for t in (count - 2, count - 1):
            for c in stores(t):
                c.wait()

    def near_arrived(first, end):
        def wait(j, carry):
            for t in (1, 3, 5, 7):
                arrived(flip(t), j)
            return carry

        lax.fori_loop(first, end, wait, 0)

    def own_done(j):
        for kind, dev in enumerate((near, across_x, across_y)):
            own(j, kind, dev).wait_send()
        store_own(j).wait()

    relay_second(last - 2)
    near_arrived(0, chips)
    caches(10, lambda t: (t // chips, t % chips))
    relay_first(last)
    caches(6, lambda t: ((t + 10) // chips, (t + 10) % chips))

    relay_second(last - 1)
    relay_second(last)
    own_done(last - 1)
    own_done(last)
    near_arrived(chips, n_dev)

    def drain(j, carry):
        forward(across_x, j, near, 0).wait_send()
        forward(across_y, j, near, 1).wait_send()
        forward(across_x, j, across_y, 2).wait_send()
        forward(diag, j, near, 3).wait_send()
        return carry

    lax.fori_loop(0, n_dev, drain, 0)
    for w in (0, 1):
        for t in (1, 2, 3):
            x_copy(w, t).wait_send()


def cache_kernel(
    kp_hbm, vp_hbm, y_hbm, wk_ref, wv_ref, bv_ref, k_hbm, v_hbm,
    wt, bias, y_s, kept_s, new_s, y_sem, kept_sem, new_sem,
):
    layers, _, cols = wk_ref.shape
    chips, frames, _ = y_s.shape
    pieces = new_sem.shape[1]
    piece = frames // pieces
    y_in = [
        [
            pltpu.make_async_copy(
                y_hbm.at[chips + i, pl.ds(p * piece, piece)], y_s.at[i, pl.ds(p * piece, piece)], y_sem.at[i, p]
            )
            for p in range(pieces)
        ]
        for i in range(chips)
    ]
    moves = [
        [
            (
                pltpu.make_async_copy(src.at[:, i], kept_s.at[i, n], kept_sem.at[0, i, n]),
                pltpu.make_async_copy(kept_s.at[i, n], dst.at[:, i], kept_sem.at[1, i, n]),
            )
            for n, (src, dst) in enumerate(((kp_hbm, k_hbm), (vp_hbm, v_hbm)))
        ]
        for i in range(chips)
    ]

    def new(i, p, n):
        at = pl.ds(p * piece, piece)
        dst = (k_hbm, v_hbm)[n]
        return pltpu.make_async_copy(new_s.at[i, n, :, :, at], dst.at[:, chips + i, :, at], new_sem.at[i, p, n])

    y_in, moves = sum(y_in, []), sum(moves, [])
    ahead, lag = 3, 2
    for c in y_in[:ahead]:
        c.start()
    cache_weights(wk_ref, wv_ref, bv_ref, wt, bias)
    for t in range(chips * pieces):
        i, p = t // pieces, t % pieces
        at = slice(p * piece, (p + 1) * piece)
        y_in[t].wait()
        if t + ahead < len(y_in):
            y_in[t + ahead].start()
        for m in range(t * len(moves) // len(y_in), (t + 1) * len(moves) // len(y_in)):
            moves[m][0].start()
        for n, x in enumerate(cache_rows(y_s[i, at], wt, bias)):
            for l in range(layers):
                new_s[i, n, l, :, at] = x[l * cols : (l + 1) * cols]
            new(i, p, n).start()
        if t >= lag:
            for m in range((t - lag) * len(moves) // len(y_in), (t - lag + 1) * len(moves) // len(y_in)):
                moves[m][0].wait()
                moves[m][1].start()
    for m in range((len(y_in) - lag) * len(moves) // len(y_in), len(moves)):
        moves[m][0].wait()
        moves[m][1].start()
    for _, store in moves:
        store.wait()
    for i in range(chips):
        for p in range(pieces):
            for n in (0, 1):
                new(i, p, n).wait()


def solution(mesh):
    n_dev = mesh.shape["sp"]

    def device_fn(x, ln1_gain, ln1_bias, w_query, b_query, w_key, w_value, b_value, w_out, b_out, ln2_gain, ln2_bias, w_up, b_up, w_down, b_down, lnp_gain, lnp_bias, cross_wk, cross_wv, cross_bv):
        clips, rows, d_model = x.shape
        d_ff = w_up.shape[1]
        frames = rows * n_dev
        layers, _, cols = cross_wk.shape
        pairs = d_model // 128
        row = lambda a: a
        hbm = pl.BlockSpec(memory_space=pl.ANY)
        vmem = pl.BlockSpec(memory_space=pltpu.VMEM)
        dma = pltpu.SemaphoreType.DMA
        shape = (layers, clips, cols, frames)
        chips = n_dev // 2
        chunk = 2 * rows
        y_all, k_part, v_part = pl.pallas_call(
            functools.partial(encoder_kernel, n_dev=n_dev, rows=rows),
            out_shape=[jax.ShapeDtypeStruct((clips, frames, d_model), BF16)] + [jax.ShapeDtypeStruct(shape, BF16)] * 2,
            in_specs=[hbm] * 9 + [vmem] * 12,
            out_specs=[hbm] * 3,
            scratch_shapes=[
                pltpu.VMEM((2, n_dev // 2, rows, d_model), BF16),
                pltpu.VMEM((d_model, d_model), BF16),
                pltpu.VMEM((d_model, d_model), BF16),
                pltpu.VMEM((d_model, d_model), BF16),
                pltpu.VMEM((d_model, d_model), BF16),
                pltpu.VMEM((d_model, d_ff), BF16),
                pltpu.VMEM((d_ff, d_model), BF16),
                pltpu.VMEM((2 * pairs, 128, frames // 2), BF16),
                pltpu.VMEM((pairs, frames, 128), BF16),
                pltpu.VMEM((2 * pairs, V_ROWS, frames), BF16),
                pltpu.VMEM((2, frames, rows), F32),
                pltpu.VMEM((2, frames, rows), F32),
                pltpu.VMEM((2, 2, 8, rows), F32),
                pltpu.VMEM((d_model, rows), BF16),
                pltpu.VMEM((2, rows, d_model), BF16),
                pltpu.VMEM((layers, d_model, cols), BF16),
                pltpu.VMEM((layers, d_model, cols), BF16),
                pltpu.VMEM((2 * layers * cols, d_model), BF16),
                pltpu.VMEM((layers * cols, cols), F32),
                pltpu.VMEM((4, chunk, d_model), BF16),
                pltpu.VMEM((2, 2, layers, cols, chunk), BF16),
                dma((2, n_dev // 2)),
                dma((2, n_dev // 2)),
                dma((2, n_dev // 2)),
                dma((2, n_dev // 2)),
                pltpu.SemaphoreType.REGULAR,
                dma((3, 2)),
                dma((4, n_dev)),
                dma((n_dev, n_dev)),
                dma((10,)),
                dma((2,)),
                dma((4,)),
                dma((2, 2)),
            ],
            compiler_params=pltpu.CompilerParams(
                collective_id=0, has_side_effects=True, vmem_limit_bytes=67043328,
            ),
            name="encoder",
        )(
            x, w_query, w_key, w_value, w_out, w_up, w_down, cross_wk, cross_wv,
            row(ln1_gain), row(ln1_bias), row(b_query), row(b_value), row(b_out), row(ln2_gain), row(ln2_bias),
            row(b_up), row(b_down), row(lnp_gain), row(lnp_bias), cross_bv,
        )
        pieces = 2
        k, v = pl.pallas_call(
            cache_kernel,
            out_shape=[jax.ShapeDtypeStruct(shape, BF16)] * 2,
            in_specs=[hbm] * 3 + [vmem] * 3,
            out_specs=[hbm] * 2,
            scratch_shapes=[
                pltpu.VMEM((2 * layers * cols, d_model), BF16),
                pltpu.VMEM((layers * cols, cols), F32),
                pltpu.VMEM((chips, frames, d_model), BF16),
                pltpu.VMEM((chips, 2, layers, cols, frames), BF16),
                pltpu.VMEM((chips, 2, layers, cols, frames), BF16),
                dma((chips, pieces)),
                dma((2, chips, 2)),
                dma((chips, pieces, 2)),
            ],
            compiler_params=pltpu.CompilerParams(vmem_limit_bytes=67043328),
            name="caches",
        )(k_part, v_part, y_all, cross_wk, cross_wv, cross_bv)
        heads = lambda a: a.reshape(layers, clips, cols // HEAD_DIM, HEAD_DIM, frames).transpose(0, 1, 4, 2, 3)
        return heads(k), heads(v)

    in_specs = (P("dp", "sp", None),) + (P(),) * 17 + (P(None, None, "sp"), P(None, None, "sp"), P(None, "sp"))
    out_specs = (P(None, "dp", None, "sp", None), P(None, "dp", None, "sp", None))
    return jax.shard_map(device_fn, mesh=mesh, in_specs=in_specs, out_specs=out_specs, check_vma=False)
```
